256 devices in a mesh: ctx: 64 (over x, z, core), dp: 4 (over y).
Axes of the slice: x: 4, y: 4, z: 8, core: 2. Of those that a mesh axis runs over, the one named last changes fastest.
Arguments:
- head_input: bfloat16 [65536, 4096], P(('dp', 'ctx')), parts along dimension 0, may hold values from -6 to 6
- gate_input: bfloat16 [65536, 4096], P(('dp', 'ctx')), parts along dimension 0, may hold values from -6 to 6
- write_vector: bfloat16 [65536, 128], P(('dp', 'ctx')), parts along dimension 0, may hold values from -2.5 to 2.5
- read_vector: bfloat16 [65536, 128], P(('dp', 'ctx')), parts along dimension 0, may hold values from -2.5 to 2.5
- increment_preactivation: bfloat16 [65536, 64], P(('dp', 'ctx')), parts along dimension 0, may hold values from -2 to 8
- step_bias: float32 [64], replicated, may hold values from -1 to 0.5
- decay_log: float32 [64], replicated, may hold values from -9.3 to -2.3
- skip_gain: float32 [64], replicated, may hold values from 0.5 to 1.5
- norm_weight: float32 [4096], replicated, may hold values from 0.5 to 1.5
- doc_starts: int32 [512], P(('dp', 'ctx')), parts along dimension 0, may hold values from 0 to 1, as said below
- block_order: int32 [512], P(('dp', 'ctx')), parts along dimension 0, may hold values from 0 to 127, as said below
Outputs:
- packed_out: bfloat16 [65536, 4096], P(('dp', 'ctx')), parts along dimension 0
The draws below stay inside these ranges and needn't reach their ends.
There are 4 independent parts, one for each index of `dp`. The reference program is written for one: setup_inputs(seed, part) draws one part's arguments, and reference() takes and returns one part's arrays. A program takes and returns all parts, laid end to end along the dimension named above; an argument that names none is the same for every part. Nothing has to cross between parts.
Inputs may be any that keep to these rules, and one draw needn't show every extreme that they name: `doc_starts`: block 0 starts a document; no document is longer than 128 blocks. `block_order`: a permutation of the block indices that keeps each document's blocks together and in their order.
All inputs are finite; a program needn't handle non-finite values.
Results may differ from the reference program's by a relative error of at most 0.0085.
Values may be sent and summed in bfloat16 or wider, within the bound.
A program may use at most 128 MiB of HBM per device.

```python
import math
import jax
import jax.numpy as jnp
from jax import lax

HEADS = 64
HEAD_DIM = 64
STATE = 128
GROUP = 128
DOC_MOST = 128
JOINED_TERMS = 16384


def doc_tables(key):
    key_baseline = jax.random.fold_in(key, 7)
    key_start, key_rank, key_extra = jax.random.split(key_baseline, 3)
    block_count = JOINED_TERMS // GROUP
    positions = jnp.arange(block_count, dtype=jnp.int32)
    chosen = jax.random.randint(key_start, (block_count,), 0, 64) == 0
    extra_at = jax.random.randint(key_extra, (4,), 1, block_count)
    hit_extra = jnp.any(positions[:, None] == extra_at[None, :], axis=1)
    forced = jnp.logical_or(positions % DOC_MOST == 0, hit_extra)
    starts = jnp.logical_or(chosen, forced).astype(jnp.int32)
    segment_number = jnp.cumsum(starts) - 1
    ranks = jax.random.randint(key_rank, (block_count,), 0, 1 << 20)
    priority = ranks[segment_number] * block_count + positions
    permuted = jnp.argsort(priority, stable=True).astype(jnp.int32)
    return (starts, permuted)


def draw_doc_starts(key, part):
    return doc_tables(key)[0]


def draw_block_order(key, part):
    return doc_tables(key)[1]


def draw_increment_preactivation(key, part):
    key_baseline = jax.random.fold_in(key, 11)
    key_value_product, lookup_jump = jax.random.split(key_baseline)
    spike_series = (jax.random.randint(lookup_jump, (JOINED_TERMS, 1), 0, 64) == 0).astype(jnp.float32)
    payload_reference_level = jnp.clip(0.5 * jax.random.normal(key_value_product, (JOINED_TERMS, HEADS), jnp.float32), -2.0, 2.0)
    return (payload_reference_level + 6.0 * spike_series).astype(jnp.bfloat16)


def draw_decay_log(key, part):
    key_baseline = jax.random.fold_in(key, 13)
    return jax.random.uniform(key_baseline, (HEADS,), jnp.float32, math.log(0.0003), math.log(0.1))


def levels(own_key, dims, shards, low, largest):
    gain = 1.0
    for axis_at, blocks in shards:
        steps = jax.random.uniform(jax.random.fold_in(jax.random.fold_in(own_key, 6), axis_at), (blocks,), jnp.float32, low / len(shards), largest / len(shards))
        gain = gain * jnp.repeat(jnp.exp(steps), dims[axis_at] // blocks).reshape((-1,) + (1,) * (len(dims) - 1 - axis_at))
    return gain


def noise(stream_key, extent, scale, reach, cuts=(), kind=jnp.bfloat16):
    entries = scale * jax.random.normal(stream_key, extent, jnp.float32)
    if cuts:
        entries = entries * levels(stream_key, extent, cuts, -0.22, 0.18)
    return jnp.clip(entries, -reach, reach).astype(kind)


def setup_inputs(seed: int = 0, part: int = 0) -> dict:
    streams_of = jax.random.split(jax.random.key(seed), 12)
    part_keys = jax.random.split(jax.random.fold_in(streams_of[11], part), 12)
    return {
        "head_input": noise(part_keys[0], (JOINED_TERMS, HEADS * HEAD_DIM), 1.0, 6.0, ((0, 64),)),
        "gate_input": noise(part_keys[1], (JOINED_TERMS, HEADS * HEAD_DIM), 1.0, 6.0, ((0, 64),)),
        "write_vector": noise(part_keys[2], (JOINED_TERMS, STATE), 0.3, 2.5, ((0, 64),)),
        "read_vector": noise(part_keys[3], (JOINED_TERMS, STATE), 0.3, 2.5, ((0, 64),)),
        "increment_preactivation": draw_increment_preactivation(jax.random.fold_in(jax.random.fold_in(streams_of[11], part), 71), part),
        "step_bias": jnp.clip(jax.random.uniform(streams_of[5], (HEADS,), jnp.float32, -1.0, 0.5), -1.0, 0.5),
        "decay_log": draw_decay_log(jax.random.fold_in(streams_of[11], 71), part),
        "skip_gain": jnp.clip(jax.random.uniform(streams_of[7], (HEADS,), jnp.float32, 0.5, 1.5), 0.5, 1.5),
        "norm_weight": jnp.clip(1.0 + 0.1 * jax.random.normal(streams_of[8], (HEADS * HEAD_DIM,), jnp.float32), 0.5, 1.5),
        "doc_starts": draw_doc_starts(jax.random.fold_in(jax.random.fold_in(streams_of[11], part), 71), part),
        "block_order": draw_block_order(jax.random.fold_in(jax.random.fold_in(streams_of[11], part), 71), part),
    }


highest = lax.Precision.HIGHEST

def product(form, left, right):
    return jnp.einsum(form, left.astype(jnp.float32), right.astype(jnp.float32), precision=highest)

def link_maps(earlier, current):
    decay_one, state_one = earlier
    decay_two, state_two = current
    return (decay_one * decay_two, decay_two[..., None, None] * state_one + state_two)

def group_terms(inputs, step_size, decay_speed, scores, write_vector, keep_mask, group_size):
    length, local_heads, head_width = inputs.shape
    group_count = length // group_size
    blocked = inputs.reshape(group_count, group_size, local_heads, head_width)
    steps_blocked = step_size.reshape(group_count, group_size, local_heads).transpose(0, 2, 1)
    cumulative = jnp.cumsum(-steps_blocked * decay_speed[None, :, None], axis=2)
    row_labels = lax.broadcasted_iota(jnp.int32, (group_size, group_size), 0)
    col_ids = lax.broadcasted_iota(jnp.int32, (group_size, group_size), 1)
    gap_log = cumulative[:, :, :, None] - cumulative[:, :, None, :]
    decays = jnp.exp(jnp.where(row_labels >= col_ids, gap_log, -jnp.inf))
    weight = (scores[:, None, :, :] * decays * steps_blocked[:, :, None, :]).astype(jnp.bfloat16)
    local_out = product('chij,cjhp->cihp', weight, blocked)
    last_cum = cumulative[:, :, -1]
    tail_decay = jnp.exp(last_cum[:, :, None] - cumulative) * steps_blocked
    scaled = (blocked.astype(jnp.float32) * tail_decay.transpose(0, 2, 1)[..., None]).astype(jnp.bfloat16)
    write_blocked = write_vector.reshape(group_count, group_size, -1)
    states = product('cjhp,cjn->chpn', scaled, write_blocked)
    factor = jnp.exp(last_cum) * keep_mask[:, None]
    scan_decay, scan_state = lax.associative_scan(link_maps, (factor, states))
    return (local_out, cumulative, scan_decay, scan_state)

def finish_groups(local_out, cumulative, scan_decay, scan_state, keep_mask, read_vector, starting_entry, inputs, skip_gain):
    group_count, group_size, local_heads, head_width = local_out.shape
    prior_decay = jnp.concatenate([jnp.ones((1, local_heads), jnp.float32), scan_decay[:-1]], 0)
    prior_state = jnp.concatenate([jnp.zeros((1,) + scan_state.shape[1:], jnp.float32), scan_state[:-1]], 0)
    entering = keep_mask[:, None, None, None] * (prior_decay[:, :, None, None] * starting_entry[None] + prior_state)
    read_blocked = read_vector.reshape(group_count, group_size, -1)
    carried = product('cin,chpn->cihp', read_blocked, entering)
    carried = carried * jnp.exp(cumulative).transpose(0, 2, 1)[..., None]
    blocked = inputs.reshape(local_out.shape).astype(jnp.float32)
    result = local_out + carried + skip_gain[None, None, :, None] * blocked
    return result.reshape(group_count * group_size, local_heads * head_width)

def gated_norm(gated, norm_weight):
    values = gated.astype(jnp.float32)
    mean_square = lax.optimization_barrier(jnp.mean(values * values, axis=-1, keepdims=True))
    return (values * lax.rsqrt(mean_square + 1e-05) * norm_weight).astype(jnp.bfloat16)

def reference(head_input, gate_input, write_vector, read_vector, increment_preactivation, step_bias, decay_log, skip_gain, norm_weight, doc_starts, block_order):
    step_size = jax.nn.softplus(increment_preactivation.astype(jnp.float32) + step_bias)
    decay_speed = jnp.exp(decay_log)
    keep_mask = 1.0 - doc_starts.astype(jnp.float32)
    group_count = JOINED_TERMS // GROUP
    scores = product('cin,cjn->cij', read_vector.reshape(group_count, GROUP, -1), write_vector.reshape(group_count, GROUP, -1))
    per_head = head_input.reshape(JOINED_TERMS, HEADS, HEAD_DIM).transpose(1, 0, 2)[:, :, None, :]

    def one_head(pieces):
        inputs, head_steps, attention_forgetting, head_gain = pieces
        local_out, cumulative, scan_decay, scan_state = group_terms(inputs, head_steps[:, None], attention_forgetting[None], scores, write_vector, keep_mask, GROUP)
        starting_entry = jnp.zeros((1, HEAD_DIM, STATE), jnp.float32)
        return finish_groups(local_out, cumulative, scan_decay, scan_state, keep_mask, read_vector, starting_entry, inputs, head_gain[None])
    outputs = lax.map(one_head, (per_head, step_size.T, decay_speed, skip_gain))
    combined = outputs.transpose(1, 0, 2).reshape(JOINED_TERMS, HEADS * HEAD_DIM)
    gated = (combined * jax.nn.silu(gate_input.astype(jnp.float32))).astype(jnp.bfloat16)
    normed = gated_norm(gated, norm_weight)
    return normed.reshape(group_count, GROUP, -1)[block_order].reshape(JOINED_TERMS, HEADS * HEAD_DIM)
```

```python
import functools

import jax
import jax.numpy as jnp
from jax import lax
from jax.experimental import pallas as pl
from jax.experimental.pallas import tpu as pltpu
from jax.sharding import PartitionSpec as P

GROUP = 128
HEAD_DIM = 64
STATE = 128
LANES = 128
LOG2E = 1.4426950408889634
F32 = jnp.float32
BF16 = jnp.bfloat16
MESH = pl.DeviceIdType.MESH


def high(v):
    return v.astype(BF16).astype(F32)


def split2(v):
    hi = high(v)
    return hi.astype(BF16), (v - hi).astype(BF16)


def split3(v):
    hi = high(v)
    mid = high(v - hi)
    return hi.astype(BF16), mid.astype(BF16), (v - hi - mid).astype(BF16)


def dot(a, b):
    return jnp.dot(a, b, preferred_element_type=F32)


def iota(shape, dim):
    return lax.broadcasted_iota(jnp.int32, shape, dim)


def picks_two(k):
    shape = (2 * HEAD_DIM, LANES)
    return ((iota(shape, 0) & 63) == 2 * k + (iota(shape, 1) >> 6)).astype(BF16)


def picks_three(k):
    shape = (192, 2 * LANES)
    return ((iota(shape, 0) & 63) == 2 * k + (iota(shape, 1) >> 7)).astype(BF16)


def local_kernel(starts_ref, x_ref, b_ref, c_ref, inc_ref, par_ref,
                 m_ref, s0_ref, f_ref, d_ref, e2_ref, col_s, exp_s, row_s, bt_s, sc_s):
    pairs = x_ref.shape[1] // LANES
    par = par_ref[...]
    bias, rate, skip = par[0:1, :], jnp.exp(par[1:2, :]), par[2:3, :]
    v = inc_ref[...].astype(F32) + bias
    step = jnp.maximum(v, 0.0) + jnp.log(1.0 + jnp.exp(-jnp.abs(v)))
    fall = -step * rate
    tri = (iota((GROUP, GROUP), 0) >= iota((GROUP, GROUP), 1))
    ones = tri.astype(F32)
    logs = []
    decs = []
    for b in range(2):
        rows = slice(b * GROUP, (b + 1) * GROUP)
        st = step[rows, :]
        cum = jnp.dot(ones, fall[rows, :], preferred_element_type=F32, precision=lax.Precision.HIGHEST)
        last = cum[GROUP - 1:GROUP, :]
        keep = 1.0 - starts_ref[b].astype(F32)
        decs.append(keep * jnp.exp(last))
        td = jnp.exp(last - cum) * st
        exp_s[rows, :] = jnp.concatenate(split2(td), axis=1)
        ec = jnp.concatenate(split2(jnp.exp(cum)), axis=1)
        exp_s[pl.ds(256 + b * GROUP, GROUP), :] = ec
        col_s[rows, :] = jnp.concatenate(split3(cum * LOG2E), axis=1)
        logs.append((jnp.log(st) - cum) * LOG2E)
        bb = b_ref[rows, :]
        bt_s[rows, :] = bb.astype(F32).T.astype(BF16)
        sc_s[rows, :] = lax.dot_general(c_ref[rows, :], bb, (((1,), (1,)), ((), ())), preferred_element_type=F32)
    row_s[...] = jnp.concatenate(logs, axis=1).T
    r16 = iota((16, HEAD_DIM), 0)
    small = jnp.where(r16 == 0, decs[0], jnp.where(r16 == 1, decs[1], jnp.where(r16 == 2, skip, 0.0)))
    small = jnp.concatenate(split2(small), axis=1)
    exp_s[pl.ds(512, 16), :] = small
    e2_ref[...] = exp_s[pl.ds(256, 272), :]

    def pair(k, carry):
        lanes = pl.ds(pl.multiple_of(k * LANES, LANES), LANES)
        col = dot(col_s[...], picks_three(k))
        ex = dot(exp_s[...], picks_two(k))
        a0, a1, gain = ex[512:513, :], ex[513:514, :], ex[514:515, :]
        left = iota((GROUP, LANES), 1) < HEAD_DIM
        states = []
        for b in range(2):
            rows = slice(b * GROUP, (b + 1) * GROUP)
            xb = x_ref[rows, lanes]
            xf = xb.astype(F32)
            scaled = (xf * ex[rows, :]).astype(BF16)
            states.append(dot(bt_s[rows, :], scaled))
            outs = []
            for e in range(2):
                gap = col[rows, e * LANES:(e + 1) * LANES] + row_s[pl.ds(b * HEAD_DIM + 2 * k + e, 1), :]
                w = jnp.exp2(jnp.where(tri, gap, -1e30)) * sc_s[rows, :]
                outs.append(dot(w.astype(BF16), xb))
            m_ref[rows, lanes] = (jnp.where(left, outs[0], outs[1]) + gain * xf).astype(BF16)
        s0_ref[:, lanes] = states[0].astype(BF16)
        f_ref[:, lanes] = (a1 * states[0] + states[1]).astype(BF16)
        d_ref[pl.ds(k, 1)] = (a0 * a1).reshape(1, 1, LANES)
        return carry

    lax.fori_loop(0, pairs, pair, 0)


def finish_kernel(starts_ref, g_ref, s0_ref, m_ref, gate_ref, c_ref, e2_ref, out_ref):
    pairs = m_ref.shape[1] // LANES
    keep0 = 1.0 - starts_ref[0].astype(F32)
    keep1 = 1.0 - starts_ref[1].astype(F32)

    def pair(k, carry):
        lanes = pl.ds(pl.multiple_of(k * LANES, LANES), LANES)
        ex = dot(e2_ref[...], picks_two(k))
        g = g_ref[:, lanes].astype(F32)
        after = ex[256:257, :] * g + s0_ref[:, lanes].astype(F32)
        entering = ((keep0 * g).astype(BF16), (keep1 * after).astype(BF16))
        for b in range(2):
            rows = slice(b * GROUP, (b + 1) * GROUP)
            carried = dot(c_ref[rows, :], entering[b])
            mixed = m_ref[rows, lanes].astype(F32) + ex[rows, :] * carried
            z = gate_ref[rows, lanes].astype(F32)
            out_ref[rows, lanes] = (mixed * (z / (1.0 + jnp.exp(-z)))).astype(BF16)
        return carry

    lax.fori_loop(0, pairs, pair, 0)


def greet(n):
    me = lax.axis_index("ctx")
    barrier = pltpu.get_barrier_semaphore()

    def one(t, carry):
        pl.semaphore_signal(barrier, inc=1, device_id={"ctx": lax.rem(me + t, n)}, device_id_type=MESH)
        return carry

    lax.fori_loop(1, n, one, 0)
    pl.semaphore_wait(barrier, n - 1)


def remote(src, dst, send, recv, device):
    return pltpu.make_async_remote_copy(
        src_ref=src, dst_ref=dst, send_sem=send, recv_sem=recv,
        device_id={"ctx": device}, device_id_type=MESH)


def order_of(i, n):
    return jnp.where((i & 1) == 1, (i + 1) // 2, n - i // 2)


def scan_kernel(n, f_ref, d_ref, g_ref, pf, pd, fc, dc, rf, rd, gs, gh, ssem, rsem, bsend, brecv):
    me = lax.axis_index("ctx")
    chip, core = me // 2, me % 2
    chips = n // 2
    other = chip * 2 + (1 - core)
    greet(n)
    swap_f = remote(f_ref, pf, ssem.at[0], rsem.at[0], other)
    swap_d = remote(d_ref, pd, ssem.at[1], rsem.at[1], other)
    swap_f.start()
    swap_d.start()
    swap_f.wait()
    swap_d.wait()
    half = pl.ds(pl.multiple_of(core * 64, 64), 64)
    first = core == 0

    def join(k, carry):
        lanes = pl.ds(pl.multiple_of(k * LANES, LANES), LANES)
        mine, theirs = f_ref[half, lanes].astype(F32), pf[half, lanes].astype(F32)
        dm, dt = d_ref[k], pd[k]
        f0, f1 = jnp.where(first, mine, theirs), jnp.where(first, theirs, mine)
        d1 = jnp.where(first, dt, dm)
        fc[k] = (d1 * f0 + f1).astype(BF16)
        dc[k] = dm * dt
        return carry

    lax.fori_loop(0, chips, join, 0)

    def out_copies(i):
        k = lax.rem(chip + order_of(i, chips), chips)
        return (remote(fc.at[k], rf.at[chip], bsend.at[0, i], brecv.at[0, i], 2 * k + core),
                remote(dc.at[k], rd.at[chip], bsend.at[1, i], brecv.at[1, i], 2 * k + core))

    def each(lo, hi, act):
        def body(i, carry):
            act(i)
            return carry
        lax.fori_loop(lo, hi, body, 0)

    def start_all(make):
        def act(i):
            for copy in make(i):
                copy.start()
        each(1, chips, act)

    def wait_all(make):
        def act(i):
            for copy in make(i):
                copy.wait()
        each(1, chips, act)

    start_all(out_copies)
    rf[chip] = fc[chip]
    rd[chip] = dc[chip]
    wait_all(out_copies)

    def walk(s, g):
        gs[s] = g.astype(BF16)
        return rd[s] * g + rf[s].astype(F32)

    lax.fori_loop(0, chips, walk, jnp.zeros((64, LANES), F32))

    def back_copies(i):
        s = lax.rem(chip + order_of(i, chips), chips)
        return (remote(gs.at[s], gh.at[core, chip], bsend.at[2, i], brecv.at[2, i], 2 * s + core),)

    start_all(back_copies)
    gh[core, chip] = gs[chip]
    wait_all(back_copies)
    swap_g = remote(gh.at[core], gh.at[core], ssem.at[2], rsem.at[2], other)
    swap_g.start()
    swap_g.wait()

    def leave(k, carry):
        lanes = pl.ds(pl.multiple_of(k * LANES, LANES), LANES)
        d0 = pd[k]
        for a in range(2):
            rows = pl.ds(a * 64, 64)
            g = gh[a, k]
            later = (d0 * g.astype(F32) + pf[rows, lanes].astype(F32)).astype(BF16)
            g_ref[rows, lanes] = jnp.where(first, g.astype(F32), later.astype(F32)).astype(BF16)
        return carry

    lax.fori_loop(0, chips, leave, 0)


def route_kernel(n, order_ref, gated_ref, out_ref, buf, perm, send1, recv1, send2, recv2):
    me = lax.axis_index("ctx")
    chip, core = me // 2, me % 2
    greet(n)
    lanes = pl.ds(pl.multiple_of(chip * LANES, LANES), LANES)

    def piece(ref, device):
        k, c = device // 2, device % 2
        return ref.at[:, pl.ds(pl.multiple_of(c * 64, 64), 64), pl.ds(pl.multiple_of(k * LANES, LANES), LANES)]

    def go(i):
        to = lax.rem(me + order_of(i, n), n)
        return remote(piece(gated_ref, to), buf.at[pl.ds(2 * me, 2)], send1.at[i], recv1.at[i], to)

    def back(i):
        to = lax.rem(me + order_of(i, n), n)
        return remote(perm.at[pl.ds(2 * to, 2)], piece(out_ref, me), send2.at[i], recv2.at[i], to)

    def each(act):
        def body(i, carry):
            act(i)
            return carry
        lax.fori_loop(1, n, body, 0)

    each(lambda i: go(i).start())
    rows = pl.ds(pl.multiple_of(core * 64, 64), 64)
    buf[pl.ds(2 * me, 2)] = gated_ref[:, rows, lanes]
    each(lambda i: go(i).wait())

    def pick(q, carry):
        perm[q] = buf[order_ref[q]]
        return carry

    lax.fori_loop(0, 2 * n, pick, 0)
    each(lambda i: back(i).start())
    out_ref[:, rows, lanes] = perm[pl.ds(2 * me, 2)]
    each(lambda i: back(i).wait())


def norm_kernel(v_ref, w_ref, o_ref):
    v = v_ref[...].astype(F32)
    mean = jnp.mean(v * v, axis=-1, keepdims=True)
    o_ref[...] = (v * lax.rsqrt(mean + 1e-05) * w_ref[...]).astype(BF16)


def local(head_input, gate_input, write_vector, read_vector, increment_preactivation, step_bias,
          decay_log, skip_gain, norm_weight, doc_starts, block_order):
    n = lax.axis_size("ctx")
    chips = n // 2
    tokens, width = head_input.shape
    vmem = pl.BlockSpec(memory_space=pltpu.VMEM)
    smem = pl.BlockSpec(memory_space=pltpu.SMEM)
    all_order = lax.all_gather(block_order, "ctx", axis=0, tiled=True)
    par = jnp.zeros((8, HEAD_DIM), F32)
    par = jnp.concatenate([step_bias[None], decay_log[None], skip_gain[None], par[3:]], axis=0)
    m, s0, f, d, e2 = pl.pallas_call(
        local_kernel,
        out_shape=(
            jax.ShapeDtypeStruct((tokens, width), BF16),
            jax.ShapeDtypeStruct((STATE, width), BF16),
            jax.ShapeDtypeStruct((STATE, width), BF16),
            jax.ShapeDtypeStruct((chips, 1, LANES), F32),
            jax.ShapeDtypeStruct((272, 2 * HEAD_DIM), BF16),
        ),
        in_specs=[smem] + [vmem] * 5,
        out_specs=(vmem,) * 5,
        scratch_shapes=[
            pltpu.VMEM((2 * GROUP, 192), BF16),
            pltpu.VMEM((528, 2 * HEAD_DIM), BF16),
            pltpu.VMEM((2 * HEAD_DIM, GROUP), F32),
            pltpu.VMEM((2 * STATE, GROUP), BF16),
            pltpu.VMEM((2 * GROUP, GROUP), F32),
        ],
        name="local_terms",
    )(doc_starts, head_input, write_vector, read_vector, increment_preactivation, par)
    g = pl.pallas_call(
        functools.partial(scan_kernel, n),
        out_shape=jax.ShapeDtypeStruct((STATE, width), BF16),
        in_specs=[vmem] * 2,
        out_specs=vmem,
        scratch_shapes=[
            pltpu.VMEM((STATE, width), BF16),
            pltpu.VMEM((chips, 1, LANES), F32),
            pltpu.VMEM((chips, 64, LANES), BF16),
            pltpu.VMEM((chips, 1, LANES), F32),
            pltpu.VMEM((chips, 64, LANES), BF16),
            pltpu.VMEM((chips, 1, LANES), F32),
            pltpu.VMEM((chips, 64, LANES), BF16),
            pltpu.VMEM((2, chips, 64, LANES), BF16),
            pltpu.SemaphoreType.DMA((3,)),
            pltpu.SemaphoreType.DMA((3,)),
            pltpu.SemaphoreType.DMA((3, chips)),
            pltpu.SemaphoreType.DMA((3, chips)),
        ],
        compiler_params=pltpu.CompilerParams(collective_id=1, has_side_effects=True),
        name="state_scan",
    )(f, d)
    gated = pl.pallas_call(
        finish_kernel,
        out_shape=jax.ShapeDtypeStruct((tokens, width), BF16),
        in_specs=[smem] + [vmem] * 6,
        out_specs=vmem,
        name="finish_terms",
    )(doc_starts, g, s0, m, gate_input, read_vector, e2)
    routed = pl.pallas_call(
        functools.partial(route_kernel, n),
        out_shape=jax.ShapeDtypeStruct((2, GROUP, width), BF16),
        in_specs=[smem, vmem],
        out_specs=vmem,
        scratch_shapes=[
            pltpu.VMEM((2 * n, 64, LANES), BF16),
            pltpu.VMEM((2 * n, 64, LANES), BF16),
        ] + [pltpu.SemaphoreType.DMA((n,))] * 4,
        compiler_params=pltpu.CompilerParams(collective_id=2, has_side_effects=True),
        name="route_blocks",
    )(all_order, gated.reshape(2, GROUP, width))
    return pl.pallas_call(
        norm_kernel,
        out_shape=jax.ShapeDtypeStruct((tokens, width), BF16),
        grid=(8,),
        in_specs=[pl.BlockSpec((tokens // 8, width), lambda i: (i, 0)), pl.BlockSpec((1, width), lambda i: (0, 0))],
        out_specs=pl.BlockSpec((tokens // 8, width), lambda i: (i, 0)),
        name="gated_norm",
    )(routed.reshape(tokens, width), norm_weight[None])


def solution(mesh):
    return jax.shard_map(
        local,
        mesh=mesh,
        in_specs=(
            P(("dp", "ctx"), None),
            P(("dp", "ctx"), None),
            P(("dp", "ctx"), None),
            P(("dp", "ctx"), None),
            P(("dp", "ctx"), None),
            P(),
            P(),
            P(),
            P(),
            P(("dp", "ctx")),
            P(("dp", "ctx")),
        ),
        out_specs=P(("dp", "ctx"), None),
        check_vma=False,
    )
```

```python
import functools

import jax
import jax.numpy as jnp
from jax import lax
from jax.experimental import pallas as pl
from jax.experimental.pallas import tpu as pltpu
from jax.sharding import PartitionSpec as P

GROUP = 128
HEAD_DIM = 64
STATE = 128
LANES = 128
LOG2E = 1.4426950408889634
F32 = jnp.float32
BF16 = jnp.bfloat16
MESH = pl.DeviceIdType.MESH


def high(v):
    return v.astype(BF16).astype(F32)


def split2(v):
    hi = high(v)
    return hi.astype(BF16), (v - hi).astype(BF16)


def split3(v):
    hi = high(v)
    mid = high(v - hi)
    return hi.astype(BF16), mid.astype(BF16), (v - hi - mid).astype(BF16)


def dot(a, b):
    return jnp.dot(a, b, preferred_element_type=F32)


def iota(shape, dim):
    return lax.broadcasted_iota(jnp.int32, shape, dim)


def picks_two(k):
    shape = (2 * HEAD_DIM, LANES)
    return ((iota(shape, 0) & 63) == 2 * k + (iota(shape, 1) >> 6)).astype(BF16)


def picks_three(k):
    shape = (192, 2 * LANES)
    return ((iota(shape, 0) & 63) == 2 * k + (iota(shape, 1) >> 7)).astype(BF16)


def remote(src, dst, send, recv, device):
    return pltpu.make_async_remote_copy(
        src_ref=src, dst_ref=dst, send_sem=send, recv_sem=recv,
        device_id={"ctx": device}, device_id_type=MESH)


def order_of(i, n):
    return jnp.where((i & 1) == 1, (i + 1) // 2, n - i // 2)


def each(lo, hi, act, step=1):
    def body(i, carry):
        for u in range(step):
            act(lo + i * step + u)
        return carry

    lax.fori_loop(0, (hi - lo) // step, body, 0)


def mega_kernel(n, starts_ref, mine_ref, x_ref, gate_hbm, b_ref, c_ref, inc_ref, par_ref, out_ref,
                gate_v, m_s, s0_s, f_s, pf, d_s, pd, fc, dc, rf, rd, gs, gh, st1, buf, perm,
                ordrow, ordv, ordsm, col_s, exp_s, row_s, bt_s, sc_s,
                gsem, osem, swf_s, swf_r, swd_s, swd_r, out_sem, back_s, back_r, swg_s, swg_r, one_sem, two_sem):
    me = lax.axis_index("ctx")
    chip, core = me // 2, me % 2
    chips = n // 2
    last = chips - 1
    other = chip * 2 + (1 - core)
    first = core == 0

    def offset(j):
        return jnp.where(j == last, 0, order_of(j + 1, chips))

    def pair_at(j):
        return lax.rem(chip - offset(j) + chips, chips)

    def lanes_of(k):
        return pl.ds(pl.multiple_of(k * LANES, LANES), LANES)

    def half_of(c):
        return pl.ds(pl.multiple_of(c * 64, 64), 64)

    barrier = pltpu.get_barrier_semaphore()
    each(1, n, lambda t: pl.semaphore_signal(
        barrier, inc=1, device_id={"ctx": lax.rem(me + t, n)}, device_id_type=MESH))
    gate_copy = pltpu.make_async_copy(gate_hbm, gate_v, gsem.at[0])
    gate_copy.start()
    lane = iota((1, LANES), 1)
    ordrow[...] = jnp.where(lane == 0, mine_ref[0], mine_ref[1])
    ordv[me] = jnp.where(lane == 0, mine_ref[0], mine_ref[1])

    par = par_ref[...]
    bias, rate, skip = par[0:1, :], jnp.exp(par[1:2, :]), par[2:3, :]
    v = inc_ref[...].astype(F32) + bias
    step = jnp.maximum(v, 0.0) + jnp.log(1.0 + jnp.exp(-jnp.abs(v)))
    fall = -step * rate
    tri = (iota((GROUP, GROUP), 0) >= iota((GROUP, GROUP), 1))
    ones = tri.astype(F32)
    logs, decs = [], []
    keep0 = 1.0 - starts_ref[0].astype(F32)
    keep1 = 1.0 - starts_ref[1].astype(F32)
    for b in range(2):
        rows = slice(b * GROUP, (b + 1) * GROUP)
        st = step[rows, :]
        cum = jnp.dot(ones, fall[rows, :], preferred_element_type=F32, precision=lax.Precision.HIGHEST)
        end = cum[GROUP - 1:GROUP, :]
        decs.append((keep0, keep1)[b] * jnp.exp(end))
        exp_s[rows, :] = jnp.concatenate(split2(jnp.exp(end - cum) * st), axis=1)
        exp_s[pl.ds(256 + b * GROUP, GROUP), :] = jnp.concatenate(split2(jnp.exp(cum)), axis=1)
        col_s[rows, :] = jnp.concatenate(split3(cum * LOG2E), axis=1)
        logs.append((jnp.log(st) - cum) * LOG2E)
        bt_s[rows, :] = b_ref[rows, :].astype(F32).T.astype(BF16)
    r16 = iota((16, HEAD_DIM), 0)
    small = jnp.where(r16 == 0, decs[0], jnp.where(r16 == 1, decs[1], jnp.where(r16 == 2, skip, 0.0)))
    exp_s[pl.ds(512, 16), :] = jnp.concatenate(split2(small), axis=1)

    def states_of(j):
        k = pair_at(j)
        lanes = lanes_of(k)
        pick = picks_two(k)
        ex = dot(exp_s[pl.ds(0, 256), :], pick)
        ends = dot(exp_s[pl.ds(512, 16), :], pick)
        a0, a1 = ends[0:1, :], ends[1:2, :]
        states = []
        for b in range(2):
            rows = slice(b * GROUP, (b + 1) * GROUP)
            scaled = (x_ref[rows, lanes].astype(F32) * ex[rows, :]).astype(BF16)
            states.append(dot(bt_s[rows, :], scaled))
        s0_s[j] = states[0]
        f_s[j] = (a1 * states[0] + states[1]).astype(BF16)
        d_s[j] = a0 * a1

    def swap(q):
        part = pl.ds(q * 8, 8)
        return (remote(f_s.at[part], pf.at[part], swf_s.at[q], swf_r.at[q], other),
                remote(d_s.at[part], pd.at[part], swd_s.at[q], swd_r.at[q], other))

    half = half_of(core)

    def join(j):
        mine, theirs = f_s[j, half, :].astype(F32), pf[j, half, :].astype(F32)
        dm, dt = d_s[j], pd[j]
        f0, f1 = jnp.where(first, mine, theirs), jnp.where(first, theirs, mine)
        fc[j] = (jnp.where(first, dt, dm) * f0 + f1).astype(BF16)
        dc[j] = dm * dt

    def send_state(j):
        to = 2 * pair_at(j) + core
        remote(fc.at[j], rf.at[chip], out_sem.at[0], out_sem.at[1], to).start()
        remote(dc.at[j], rd.at[chip], out_sem.at[2], out_sem.at[3], to).start()

    def join_chunk(q):
        for copy in swap(q):
            copy.wait_recv()
        each(q * 8, q * 8 + 8, join, 2)
        each(q * 8, min(q * 8 + 8, last), send_state)

    for q in range(4):
        each(q * 8, q * 8 + 8, states_of, 2)
        if q == 0:
            pl.semaphore_wait(barrier, n - 1)
        else:
            join_chunk(q - 1)
        for copy in swap(q):
            copy.start()
    each(1, n, lambda t: remote(
        ordrow, ordv.at[me], osem.at[0], osem.at[1], lax.rem(me + t, n)).start())
    row_s[...] = jnp.concatenate(logs, axis=1).T
    for b in range(2):
        rows = slice(b * GROUP, (b + 1) * GROUP)
        sc_s[rows, :] = lax.dot_general(
            c_ref[rows, :], b_ref[rows, :], (((1,), (1,)), ((), ())), preferred_element_type=F32)
    join_chunk(3)
    rf[chip] = fc[last]
    rd[chip] = dc[last]

    def local_of(j):
        k = pair_at(j)
        lanes = lanes_of(k)
        col = dot(col_s[...], picks_three(k))
        gain = dot(exp_s[pl.ds(512, 16), :], picks_two(k))[2:3, :]
        left = iota((GROUP, LANES), 1) < HEAD_DIM
        for b in range(2):
            rows = slice(b * GROUP, (b + 1) * GROUP)
            xb = x_ref[rows, lanes]
            outs = []
            for e in range(2):
                gap = col[rows, e * LANES:(e + 1) * LANES] + row_s[pl.ds(b * HEAD_DIM + 2 * k + e, 1), :]
                w = jnp.exp2(jnp.where(tri, gap, -1e30)) * sc_s[rows, :]
                outs.append(dot(w.astype(BF16), xb))
            m_s[j, rows, :] = jnp.where(left, outs[0], outs[1]) + gain * xb.astype(F32)

    each(0, 16, local_of, 2)
    remote(fc.at[pl.ds(0, last)], rf.at[pl.ds(0, last)], out_sem.at[0], out_sem.at[1], other).wait()
    remote(dc.at[pl.ds(0, last)], rd.at[pl.ds(0, last)], out_sem.at[2], out_sem.at[3], other).wait()

    def walk(s, g):
        gs[s] = g.astype(BF16)
        return rd[s] * g + rf[s].astype(F32)

    lax.fori_loop(0, chips, walk, jnp.zeros((64, LANES), F32))

    def send_back(i):
        s = lax.rem(chip + offset(i), chips)
        remote(gs.at[s], gh.at[core, i], back_s.at[0], back_r.at[i], 2 * s + core).start()

    gh[core, last] = gs[chip]
    each(0, last, send_back)
    each(16, 32, local_of, 2)
    gate_copy.wait()

    def arrived(i):
        remote(gs.at[0], gh.at[core, i], back_s.at[0], back_r.at[i], other).wait_recv()

    def finish(i):
        k = pair_at(i)
        lanes = lanes_of(k)
        pick = picks_two(k)
        ex = dot(exp_s[pl.ds(256, 256), :], pick)
        a0 = dot(exp_s[pl.ds(512, 16), :], pick)[0:1, :]
        g = jnp.concatenate([gh[0, i], gh[1, i]], axis=0).astype(F32)
        g = jnp.where(first, g, pd[i] * g + pf[i].astype(F32))
        after = a0 * g + s0_s[i]
        entering = ((keep0 * g).astype(BF16), (keep1 * after).astype(BF16))
        for b in range(2):
            rows = slice(b * GROUP, (b + 1) * GROUP)
            mixed = m_s[i, rows, :] + ex[rows, :] * dot(c_ref[rows, :], entering[b])
            z = gate_v[rows, lanes].astype(F32)
            st1[i, b] = (mixed * (z / (1.0 + jnp.exp(-z)))).astype(BF16)

    def send_one(i, c):
        remote(st1.at[i, :, half_of(c), :], buf.at[pl.ds(2 * me, 2)],
               one_sem.at[0], one_sem.at[1], 2 * pair_at(i) + c).start()

    def finish_two(t):
        finish(2 * t)
        finish(2 * t + 1)

        @pl.when(t > 0)
        def _():
            for u in range(2):
                for c in range(2):
                    send_one(2 * t - 2 + u, c)

    def swap_back(q):
        part = pl.ds(q * 8, 8)
        return remote(gh.at[core, part], gh.at[core, part], swg_s.at[q], swg_r.at[q], other)

    def swapped(q):
        part = pl.ds(q * 8, 8)
        return remote(gh.at[1 - core, part], gh.at[1 - core, part], swg_s.at[q], swg_r.at[q], other)

    for q in range(4):
        each(q * 8, min(q * 8 + 8, last), arrived)
        swap_back(q).start()
        swapped(q).wait_recv()
        each(q * 4, q * 4 + 4, finish_two)
    buf[pl.ds(2 * me, 2)] = st1[last, :, half, :]
    for q in range(4):
        for copy in swap(q):
            copy.wait_send()
        swap_back(q).wait_send()
    remote(gs.at[pl.ds(0, last)], gs.at[pl.ds(0, last)], back_s.at[0], back_r.at[0], other).wait_send()
    for c in range(2):
        send_one(last - 1, c)
    remote(st1.at[last, :, half_of(1 - core), :], buf.at[pl.ds(2 * me, 2)],
           one_sem.at[0], one_sem.at[1], other).start()
    remote(ordv.at[pl.ds(0, n - 1)], ordv.at[pl.ds(0, n - 1)], osem.at[0], osem.at[1], other).wait()
    to_scalars = pltpu.make_async_copy(ordv, ordsm, gsem.at[1])
    to_scalars.start()
    to_scalars.wait()
    whole = remote(buf.at[pl.ds(0, 2 * n - 2)], buf.at[pl.ds(0, 2 * n - 2)], one_sem.at[0], one_sem.at[1], other)
    whole.wait()

    def pick_at(i):
        to = lax.rem(me + order_of(i, n), n)
        for b in range(2):
            perm[i, b] = buf[ordsm[to, 0, b]]

    def send_two(i):
        to = lax.rem(me + order_of(i, n), n)
        remote(perm.at[i], out_ref.at[:, half, lanes_of(chip)], two_sem.at[0], two_sem.at[1], to).start()

    def pick_and_send(i):
        pick_at(i)

        @pl.when(i > 1)
        def _():
            send_two(i - 1)

    each(1, n, pick_and_send)
    for b in range(2):
        out_ref[b, half, lanes_of(chip)] = buf[ordsm[me, 0, b]]
    send_two(n - 1)
    all_two = remote(perm.at[pl.ds(0, n - 1)], perm.at[pl.ds(0, n - 1)], two_sem.at[0], two_sem.at[1], other)
    all_two.wait()


def norm_kernel(v_ref, w_ref, o_ref):
    v = v_ref[...].astype(F32)
    mean = jnp.mean(v * v, axis=-1, keepdims=True)
    o_ref[...] = (v * lax.rsqrt(mean + 1e-05) * w_ref[...]).astype(BF16)


def local(head_input, gate_input, write_vector, read_vector, increment_preactivation, step_bias,
          decay_log, skip_gain, norm_weight, doc_starts, block_order):
    n = lax.axis_size("ctx")
    chips = n // 2
    tokens, width = head_input.shape
    vmem = pl.BlockSpec(memory_space=pltpu.VMEM)
    smem = pl.BlockSpec(memory_space=pltpu.SMEM)
    par = jnp.concatenate([step_bias[None], decay_log[None], skip_gain[None], jnp.zeros((5, HEAD_DIM), F32)], axis=0)
    dma = pltpu.SemaphoreType.DMA
    routed = pl.pallas_call(
        functools.partial(mega_kernel, n),
        out_shape=jax.ShapeDtypeStruct((2, GROUP, width), BF16),
        in_specs=[smem, smem, vmem, pl.BlockSpec(memory_space=pl.ANY)] + [vmem] * 4,
        out_specs=vmem,
        scratch_shapes=[
            pltpu.VMEM((tokens, width), BF16),
            pltpu.VMEM((chips, tokens, LANES), F32),
            pltpu.VMEM((chips, STATE, LANES), F32),
            pltpu.VMEM((chips, STATE, LANES), BF16),
            pltpu.VMEM((chips, STATE, LANES), BF16),
            pltpu.VMEM((chips, 1, LANES), F32),
            pltpu.VMEM((chips, 1, LANES), F32),
            pltpu.VMEM((chips, 64, LANES), BF16),
            pltpu.VMEM((chips, 1, LANES), F32),
            pltpu.VMEM((chips, 64, LANES), BF16),
            pltpu.VMEM((chips, 1, LANES), F32),
            pltpu.VMEM((chips, 64, LANES), BF16),
            pltpu.VMEM((2, chips, 64, LANES), BF16),
            pltpu.VMEM((chips, 2, GROUP, LANES), BF16),
            pltpu.VMEM((2 * n, 64, LANES), BF16),
            pltpu.VMEM((n, 2, 64, LANES), BF16),
            pltpu.VMEM((1, LANES), jnp.int32),
            pltpu.VMEM((n, 1, LANES), jnp.int32),
            pltpu.SMEM((n, 1, LANES), jnp.int32),
            pltpu.VMEM((2 * GROUP, 192), BF16),
            pltpu.VMEM((528, 2 * HEAD_DIM), BF16),
            pltpu.VMEM((2 * HEAD_DIM, GROUP), F32),
            pltpu.VMEM((2 * STATE, GROUP), BF16),
            pltpu.VMEM((2 * GROUP, GROUP), F32),
            dma((2,)), dma((2,)), dma((4,)), dma((4,)), dma((4,)), dma((4,)), dma((4,)),
            dma((1,)), dma((chips,)), dma((4,)), dma((4,)), dma((2,)), dma((2,)),
        ],
        compiler_params=pltpu.CompilerParams(
            collective_id=1, has_side_effects=True, vmem_limit_bytes=60 * 1024 * 1024),
        name="layer",
    )(doc_starts, block_order, head_input, gate_input, write_vector, read_vector, increment_preactivation, par)
    return pl.pallas_call(
        norm_kernel,
        out_shape=jax.ShapeDtypeStruct((tokens, width), BF16),
        grid=(8,),
        in_specs=[pl.BlockSpec((tokens // 8, width), lambda i: (i, 0)), pl.BlockSpec((1, width), lambda i: (0, 0))],
        out_specs=pl.BlockSpec((tokens // 8, width), lambda i: (i, 0)),
        name="gated_norm",
    )(routed.reshape(tokens, width), norm_weight[None])


def solution(mesh):
    return jax.shard_map(
        local,
        mesh=mesh,
        in_specs=(
            P(("dp", "ctx"), None),
            P(("dp", "ctx"), None),
            P(("dp", "ctx"), None),
            P(("dp", "ctx"), None),
            P(("dp", "ctx"), None),
            P(),
            P(),
            P(),
            P(),
            P(("dp", "ctx")),
            P(("dp", "ctx")),
        ),
        out_specs=P(("dp", "ctx"), None),
        check_vma=False,
    )
```

```python
import functools

import jax
import jax.numpy as jnp
from jax import lax
from jax.experimental import pallas as pl
from jax.experimental.pallas import tpu as pltpu
from jax.sharding import PartitionSpec as P

GROUP = 128
HEAD_DIM = 64
STATE = 128
LANES = 128
LOG2E = 1.4426950408889634
F32 = jnp.float32
BF16 = jnp.bfloat16
MESH = pl.DeviceIdType.MESH


def high(v):
    return v.astype(BF16).astype(F32)


def split2(v):
    hi = high(v)
    return hi.astype(BF16), (v - hi).astype(BF16)


def split3(v):
    hi = high(v)
    mid = high(v - hi)
    return hi.astype(BF16), mid.astype(BF16), (v - hi - mid).astype(BF16)


def dot(a, b):
    return jnp.dot(a, b, preferred_element_type=F32)


def iota(shape, dim):
    return lax.broadcasted_iota(jnp.int32, shape, dim)


def picks_two(k):
    shape = (2 * HEAD_DIM, LANES)
    return ((iota(shape, 0) & 63) == 2 * k + (iota(shape, 1) >> 6)).astype(BF16)


def picks_three(k):
    shape = (192, 2 * LANES)
    return ((iota(shape, 0) & 63) == 2 * k + (iota(shape, 1) >> 7)).astype(BF16)


def remote(src, dst, send, recv, device):
    return pltpu.make_async_remote_copy(
        src_ref=src, dst_ref=dst, send_sem=send, recv_sem=recv,
        device_id={"ctx": device}, device_id_type=MESH)


def order_of(i, n):
    return jnp.where((i & 1) == 1, (i + 1) // 2, n - i // 2)


def each(lo, hi, act, step=1):
    def body(i, carry):
        for u in range(step):
            act(lo + i * step + u)
        return carry

    lax.fori_loop(0, (hi - lo) // step, body, 0)


PARTS = 2
CHUNK = 4


def mega_kernel(n, starts_ref, mine_ref, x_hbm, gate_hbm, b_ref, c_ref, inc_ref, bias_ref, decay_ref, skip_ref, out_ref,
                x_ref, gate_v, m_s, s0_s, f_s, pf, d_s, pd, fc, dc, rf, rd, gs, gh, st1, buf0, buf1, perm,
                ordrow, ordv, ordsm, col_s, exp_s, row_s, tail_s, bt_s, sc_s,
                gsem, osem, swf_s, swf_r, swd_s, swd_r, out_sem, back_s, back_r, swg_s, swg_r, one_sem, two_sem):
    me = lax.axis_index("ctx")
    chip, core = me // 2, me % 2
    chips = n // 2
    last = chips - 1
    other = chip * 2 + (1 - core)
    first = core == 0

    def offset(j):
        return jnp.where(j == last, 0, order_of(j + 1, chips))

    def pair_at(j):
        return lax.rem(chip - offset(j) + chips, chips)

    def lanes_of(k):
        return pl.ds(pl.multiple_of(k * LANES, LANES), LANES)

    def half_of(c):
        return pl.ds(pl.multiple_of(c * 64, 64), 64)

    barrier = pltpu.get_barrier_semaphore()
    each(1, n, lambda t: pl.semaphore_signal(
        barrier, inc=1, device_id={"ctx": lax.rem(me + t, n)}, device_id_type=MESH))
    gate_copy = pltpu.make_async_copy(gate_hbm, gate_v, gsem.at[0])
    x_copy = pltpu.make_async_copy(x_hbm, x_ref, gsem.at[2])
    x_copy.start()
    gate_copy.start()
    lane = iota((1, LANES), 1)
    ordrow[...] = jnp.where(lane == 0, mine_ref[0], mine_ref[1])
    ordv[me] = jnp.where(lane == 0, mine_ref[0], mine_ref[1])

    bias, rate, skip = bias_ref[...], jnp.exp(decay_ref[...]), skip_ref[...]
    v = inc_ref[...].astype(F32).T + bias
    step = jnp.maximum(v, 0.0) + jnp.log(1.0 + jnp.exp(-jnp.abs(v)))
    fall = -step * rate
    tri = (iota((GROUP, GROUP), 0) >= iota((GROUP, GROUP), 1))
    ones = tri.astype(F32)
    logs, decs, tails = [], [], []
    keep0 = 1.0 - starts_ref[0].astype(F32)
    keep1 = 1.0 - starts_ref[1].astype(F32)
    for b in range(2):
        rows = slice(b * GROUP, (b + 1) * GROUP)
        st = step[rows, :]
        cum = jnp.dot(ones, fall[rows, :], preferred_element_type=F32, precision=lax.Precision.HIGHEST)
        end = cum[GROUP - 1:GROUP, :]
        decs.append((keep0, keep1)[b] * jnp.exp(end))
        tails.append(jnp.exp(end - cum) * st)
        exp_s[rows, :] = jnp.concatenate(split2(jnp.exp(cum)), axis=1)
        col_s[rows, :] = jnp.concatenate(split3(cum * LOG2E), axis=1)
        logs.append((jnp.log(st) - cum) * LOG2E)
        bt_s[rows, :] = b_ref[rows, :].astype(F32).T
    r16 = iota((16, HEAD_DIM), 0)
    small = jnp.where(r16 == 0, decs[0], jnp.where(r16 == 1, decs[1], jnp.where(r16 == 2, skip, 0.0)))
    tail_s[...] = jnp.concatenate(tails, axis=1).T
    exp_s[pl.ds(256, 16), :] = jnp.concatenate(split2(small), axis=1)

    left = iota((GROUP, LANES), 1) < HEAD_DIM
    x_copy.wait()

    def states_of(j):
        k = pair_at(j)
        lanes = lanes_of(k)
        pick = picks_two(k)
        ends = dot(exp_s[pl.ds(256, 16), :], pick)
        a0, a1 = ends[0:1, :], ends[1:2, :]
        states = []
        for b in range(2):
            rows = slice(b * GROUP, (b + 1) * GROUP)
            both = jnp.concatenate(
                [bt_s[rows, :] * tail_s[pl.ds(b * HEAD_DIM + 2 * k + e, 1), :] for e in range(2)], axis=0)
            out = dot(both.astype(BF16), x_ref[rows, lanes])
            states.append(jnp.where(left, out[:STATE], out[STATE:]))
        s0_s[j] = states[0]
        f_s[j] = (a1 * states[0] + states[1]).astype(BF16)
        d_s[j] = a0 * a1

    def swap(q):
        part = pl.ds(q * 8, 8)
        return (remote(f_s.at[part], pf.at[part], swf_s.at[q], swf_r.at[q], other),
                remote(d_s.at[part], pd.at[part], swd_s.at[q], swd_r.at[q], other))

    half = half_of(core)

    def join(j):
        mine, theirs = f_s[j, half, :].astype(F32), pf[j, half, :].astype(F32)
        dm, dt = d_s[j], pd[j]
        f0, f1 = jnp.where(first, mine, theirs), jnp.where(first, theirs, mine)
        fc[j] = (jnp.where(first, dt, dm) * f0 + f1).astype(BF16)
        dc[j] = dm * dt

    def send_state(j):
        to = 2 * pair_at(j) + core
        remote(fc.at[j], rf.at[chip], out_sem.at[0], out_sem.at[1], to).start()
        remote(dc.at[j], rd.at[chip], out_sem.at[2], out_sem.at[3], to).start()

    def join_chunk(q):
        for copy in swap(q):
            copy.wait_recv()
        each(q * 8, q * 8 + 8, join, 2)
        each(q * 8, min(q * 8 + 8, last), send_state)

    for q in range(4):
        each(q * 8, q * 8 + 8, states_of, 2)
        if q == 0:
            pl.semaphore_wait(barrier, n - 1)
        else:
            join_chunk(q - 1)
        for copy in swap(q):
            copy.start()
    each(1, n, lambda t: remote(
        ordrow, ordv.at[me], osem.at[0], osem.at[1], lax.rem(me + t, n)).start())
    row_s[...] = jnp.concatenate(logs, axis=1).T
    for b in range(2):
        rows = slice(b * GROUP, (b + 1) * GROUP)
        sc_s[rows, :] = lax.dot_general(
            c_ref[rows, :], b_ref[rows, :], (((1,), (1,)), ((), ())), preferred_element_type=F32)
    join_chunk(3)
    rf[chip] = fc[last]
    rd[chip] = dc[last]

    def local_of(j):
        k = pair_at(j)
        lanes = lanes_of(k)
        col = dot(col_s[...], picks_three(k))
        gain = dot(exp_s[pl.ds(256, 16), :], picks_two(k))[2:3, :]
        for b in range(2):
            rows = slice(b * GROUP, (b + 1) * GROUP)
            xb = x_ref[rows, lanes]
            outs = []
            for e in range(2):
                gap = col[rows, e * LANES:(e + 1) * LANES] + row_s[pl.ds(b * HEAD_DIM + 2 * k + e, 1), :]
                w = jnp.exp2(jnp.where(tri, gap, -1e30)) * sc_s[rows, :]
                outs.append(dot(w.astype(BF16), xb))
            m_s[j, rows, :] = jnp.where(left, outs[0], outs[1]) + gain * xb.astype(F32)

    each(0, 16, local_of, 2)
    remote(fc.at[pl.ds(0, last)], rf.at[pl.ds(0, last)], out_sem.at[0], out_sem.at[1], other).wait()
    remote(dc.at[pl.ds(0, last)], rd.at[pl.ds(0, last)], out_sem.at[2], out_sem.at[3], other).wait()

    def walk(s, g):
        gs[s] = g.astype(BF16)
        return rd[s] * g + rf[s].astype(F32)

    lax.fori_loop(0, chips, walk, jnp.zeros((64, LANES), F32))

    def send_back(i):
        s = lax.rem(chip + offset(i), chips)
        remote(gs.at[s], gh.at[core, i], back_s.at[0], back_r.at[i], 2 * s + core).start()

    gh[core, last] = gs[chip]
    each(0, last, send_back)
    each(16, 32, local_of, 2)
    gate_copy.wait()

    def arrived(i):
        remote(gs.at[0], gh.at[core, i], back_s.at[0], back_r.at[i], other).wait_recv()

    def finish(i):
        k = pair_at(i)
        lanes = lanes_of(k)
        pick = picks_two(k)
        ex = dot(exp_s[...], pick)
        a0 = ex[256:257, :]
        g = jnp.concatenate([gh[0, i], gh[1, i]], axis=0).astype(F32)
        g = jnp.where(first, g, pd[i] * g + pf[i].astype(F32))
        after = a0 * g + s0_s[i]
        entering = ((keep0 * g).astype(BF16), (keep1 * after).astype(BF16))
        for b in range(2):
            rows = slice(b * GROUP, (b + 1) * GROUP)
            mixed = m_s[i, rows, :] + ex[rows, :] * dot(c_ref[rows, :], entering[b])
            z = gate_v[rows, lanes].astype(F32)
            st1[i, b] = (mixed * (z / (1.0 + jnp.exp(-z)))).astype(BF16)

    size = 64 // PARTS
    bufs = (buf0, buf1)

    def cut(c, p):
        return pl.ds(pl.multiple_of(c * 64 + p * size, size), size)

    def send_one(i, c, p):
        remote(st1.at[i, :, cut(c, p), :], bufs[p].at[pl.ds(2 * me, 2)],
               one_sem.at[0, p], one_sem.at[1, p], 2 * pair_at(i) + c).start()

    def send_last(p):
        remote(st1.at[last, :, cut(1 - core, p), :], bufs[p].at[pl.ds(2 * me, 2)],
               one_sem.at[0, p], one_sem.at[1, p], other).start()

    def finish_two(t):
        finish(2 * t)
        finish(2 * t + 1)

        @pl.when(t > 0)
        def _():
            for u in range(2):
                for c in range(2):
                    send_one(2 * t - 2 + u, c, 0)

    def swap_back(q):
        part = pl.ds(q * CHUNK, CHUNK)
        return remote(gh.at[core, part], gh.at[core, part], swg_s.at[q], swg_r.at[q], other)

    def swapped(q):
        part = pl.ds(q * CHUNK, CHUNK)
        return remote(gh.at[1 - core, part], gh.at[1 - core, part], swg_s.at[q], swg_r.at[q], other)

    rounds = chips // CHUNK
    for q in range(rounds + 1):
        if q < rounds:
            each(q * CHUNK, min(q * CHUNK + CHUNK, last), arrived)
            swap_back(q).start()
        if q > 0:
            swapped(q - 1).wait_recv()
            each((q - 1) * CHUNK // 2, q * CHUNK // 2, finish_two)
    for p in range(PARTS):
        bufs[p][pl.ds(2 * me, 2)] = st1[last, :, cut(core, p), :]
    for q in range(4):
        for copy in swap(q):
            copy.wait_send()
    for q in range(rounds):
        swap_back(q).wait_send()
    remote(gs.at[pl.ds(0, last)], gs.at[pl.ds(0, last)], back_s.at[0], back_r.at[0], other).wait_send()
    for c in range(2):
        send_one(last - 1, c, 0)
    send_last(0)
    for p in range(1, PARTS):
        def rest(i):
            for c in range(2):
                send_one(i, c, p)

        each(0, last, rest)
        send_last(p)
    remote(ordv.at[pl.ds(0, n - 1)], ordv.at[pl.ds(0, n - 1)], osem.at[0], osem.at[1], other).wait()
    to_scalars = pltpu.make_async_copy(ordv, ordsm, gsem.at[1])
    to_scalars.start()
    to_scalars.wait()

    def send_two(i, p):
        to = lax.rem(me + order_of(i, n), n)
        remote(perm.at[p, i], out_ref.at[:, cut(core, p), lanes_of(chip)],
               two_sem.at[0, p], two_sem.at[1, p], to).start()

    for p in range(PARTS):
        arrivals = remote(bufs[p].at[pl.ds(0, 2 * n - 2)], bufs[p].at[pl.ds(0, 2 * n - 2)],
                          one_sem.at[0, p], one_sem.at[1, p], other)
        arrivals.wait()

        def pick_and_send(i):
            to = lax.rem(me + order_of(i, n), n)
            for b in range(2):
                perm[p, i, b] = bufs[p][ordsm[to, 0, b]]

            @pl.when(i > 1)
            def _():
                send_two(i - 1, p)

        each(1, n, pick_and_send)
        for b in range(2):
            out_ref[b, cut(core, p), lanes_of(chip)] = bufs[p][ordsm[me, 0, b]]
        send_two(n - 1, p)
    for p in range(PARTS):
        remote(perm.at[p, pl.ds(0, n - 1)], perm.at[p, pl.ds(0, n - 1)],
               two_sem.at[0, p], two_sem.at[1, p], other).wait()


def norm_kernel(v_hbm, w_ref, o_hbm, v_ref, o_v, isem, osem):
    count = isem.shape[0]
    size = v_ref.shape[0] // count

    def rows(i):
        return pl.ds(pl.multiple_of(i * size, size), size)

    def load(i):
        return pltpu.make_async_copy(v_hbm.at[rows(i)], v_ref.at[rows(i)], isem.at[i])

    def store(i):
        return pltpu.make_async_copy(o_v.at[rows(i)], o_hbm.at[rows(i)], osem.at[i])

    each(0, count, lambda i: load(i).start())

    def body(i):
        load(i).wait()
        v = v_ref[rows(i), :].astype(F32)
        mean = jnp.mean(v * v, axis=-1, keepdims=True)
        o_v[rows(i), :] = (v * lax.rsqrt(mean + 1e-05) * w_ref[...]).astype(BF16)
        store(i).start()

    each(0, count, body)
    each(0, count, lambda i: store(i).wait())


def local(head_input, gate_input, write_vector, read_vector, increment_preactivation, step_bias,
          decay_log, skip_gain, norm_weight, doc_starts, block_order):
    n = lax.axis_size("ctx")
    chips = n // 2
    tokens, width = head_input.shape
    vmem = pl.BlockSpec(memory_space=pltpu.VMEM)
    smem = pl.BlockSpec(memory_space=pltpu.SMEM)
    dma = pltpu.SemaphoreType.DMA
    routed = pl.pallas_call(
        functools.partial(mega_kernel, n),
        out_shape=jax.ShapeDtypeStruct((2, GROUP, width), BF16),
        in_specs=[smem, smem, pl.BlockSpec(memory_space=pltpu.HBM), pl.BlockSpec(memory_space=pltpu.HBM)] + [vmem] * 6,
        out_specs=vmem,
        scratch_shapes=[
            pltpu.VMEM((tokens, width), BF16),
            pltpu.VMEM((tokens, width), BF16),
            pltpu.VMEM((chips, tokens, LANES), F32),
            pltpu.VMEM((chips, STATE, LANES), F32),
            pltpu.VMEM((chips, STATE, LANES), BF16),
            pltpu.VMEM((chips, STATE, LANES), BF16),
            pltpu.VMEM((chips, 1, LANES), F32),
            pltpu.VMEM((chips, 1, LANES), F32),
            pltpu.VMEM((chips, 64, LANES), BF16),
            pltpu.VMEM((chips, 1, LANES), F32),
            pltpu.VMEM((chips, 64, LANES), BF16),
            pltpu.VMEM((chips, 1, LANES), F32),
            pltpu.VMEM((chips, 64, LANES), BF16),
            pltpu.VMEM((2, chips, 64, LANES), BF16),
            pltpu.VMEM((chips, 2, GROUP, LANES), BF16),
            pltpu.VMEM((2 * n, 64 // PARTS, LANES), BF16),
            pltpu.VMEM((2 * n, 64 // PARTS, LANES), BF16),
            pltpu.VMEM((PARTS, n, 2, 64 // PARTS, LANES), BF16),
            pltpu.VMEM((1, LANES), jnp.int32),
            pltpu.VMEM((n, 1, LANES), jnp.int32),
            pltpu.SMEM((n, 1, LANES), jnp.int32),
            pltpu.VMEM((2 * GROUP, 192), BF16),
            pltpu.VMEM((272, 2 * HEAD_DIM), BF16),
            pltpu.VMEM((2 * HEAD_DIM, GROUP), F32),
            pltpu.VMEM((2 * HEAD_DIM, GROUP), F32),
            pltpu.VMEM((2 * STATE, GROUP), F32),
            pltpu.VMEM((2 * GROUP, GROUP), F32),
            dma((3,)), dma((2,)), dma((4,)), dma((4,)), dma((4,)), dma((4,)), dma((4,)),
            dma((1,)), dma((chips,)), dma((chips // CHUNK,)), dma((chips // CHUNK,)), dma((2, PARTS)), dma((2, PARTS)),
        ],
        compiler_params=pltpu.CompilerParams(
            collective_id=1, has_side_effects=True, vmem_limit_bytes=58 * 1024 * 1024),
        name="layer",
    )(doc_starts, block_order, head_input, gate_input, write_vector, read_vector, increment_preactivation.T,
      step_bias[None], decay_log[None], skip_gain[None])
    return pl.pallas_call(
        norm_kernel,
        out_shape=jax.ShapeDtypeStruct((tokens, width), BF16),
        in_specs=[pl.BlockSpec(memory_space=pl.ANY), vmem],
        out_specs=pl.BlockSpec(memory_space=pl.ANY),
        scratch_shapes=[pltpu.VMEM((tokens, width), BF16)] * 2 + [dma((8,)), dma((8,))],
        compiler_params=pltpu.CompilerParams(vmem_limit_bytes=58 * 1024 * 1024),
        name="gated_norm",
    )(routed.reshape(tokens, width), norm_weight[None])


def solution(mesh):
    return jax.shard_map(
        local,
        mesh=mesh,
        in_specs=(
            P(("dp", "ctx"), None),
            P(("dp", "ctx"), None),
            P(("dp", "ctx"), None),
            P(("dp", "ctx"), None),
            P(("dp", "ctx"), None),
            P(),
            P(),
            P(),
            P(),
            P(("dp", "ctx")),
            P(("dp", "ctx")),
        ),
        out_specs=P(("dp", "ctx"), None),
        check_vma=False,
    )
```

```python
import functools

import jax
import jax.numpy as jnp
from jax import lax
from jax.experimental import pallas as pl
from jax.experimental.pallas import tpu as pltpu
from jax.sharding import PartitionSpec as P

GROUP = 128
HEAD_DIM = 64
STATE = 128
LANES = 128
LOG2E = 1.4426950408889634
F32 = jnp.float32
BF16 = jnp.bfloat16
MESH = pl.DeviceIdType.MESH


def high(v):
    return v.astype(BF16).astype(F32)


def split2(v):
    hi = high(v)
    return hi.astype(BF16), (v - hi).astype(BF16)


def split3(v):
    hi = high(v)
    mid = high(v - hi)
    return hi.astype(BF16), mid.astype(BF16), (v - hi - mid).astype(BF16)


def dot(a, b):
    return jnp.dot(a, b, preferred_element_type=F32)


def iota(shape, dim):
    return lax.broadcasted_iota(jnp.int32, shape, dim)


def picks_two(k):
    shape = (2 * HEAD_DIM, LANES)
    return ((iota(shape, 0) & 63) == 2 * k + (iota(shape, 1) >> 6)).astype(BF16)


def picks_three(k):
    shape = (192, 2 * LANES)
    return ((iota(shape, 0) & 63) == 2 * k + (iota(shape, 1) >> 7)).astype(BF16)


def remote(src, dst, send, recv, device):
    return pltpu.make_async_remote_copy(
        src_ref=src, dst_ref=dst, send_sem=send, recv_sem=recv,
        device_id={"ctx": device}, device_id_type=MESH)


def around(i, n):
    return jnp.where(i == n - 1, 0, jnp.where((i & 1) == 0, i // 2 + 1, n - (i + 1) // 2))


def each(lo, hi, act, step=1):
    def body(i, carry):
        for u in range(step):
            act(lo + i * step + u)
        return carry

    lax.fori_loop(0, (hi - lo) // step, body, 0)


PARTS = 2
W0, W1 = 12, 22
CHUNK = 2


def mega_kernel(n, starts_hbm, mine_hbm, x_hbm, gate_hbm, b_ref, c_ref, inc_ref, bias_ref, decay_ref, skip_ref, out_ref,
                starts_ref, mine_ref, x_ref, gate_v, m_s, s0_s, f_s, pf, d_s, pd, fc, dc, rf, rd, gs, gh, st1, buf0, buf1, perm,
                ordrow, ordv, ordsm, col_s, exp_s, row_s, tail_s, bt_s, sc_s,
                gsem, osem, swf_s, swf_r, swd_s, swd_r, out_sem, back_s, back_r, swg_s, swg_r, one_sem, two_sem):
    me = lax.axis_index("ctx")
    chip, core = me // 2, me % 2
    chips = n // 2
    last = chips - 1
    other = chip * 2 + (1 - core)
    first = core == 0

    def shifted(j, sign):
        return lax.rem(chip + sign * around(j, chips) + chips, chips)

    def pair_at(j):
        return shifted(j, -1)

    def device_at(i):
        return lax.rem(me + around(i, n), n)

    def lanes_of(k):
        return pl.ds(pl.multiple_of(k * LANES, LANES), LANES)

    def half_of(c):
        return pl.ds(pl.multiple_of(c * 64, 64), 64)

    barrier = pltpu.get_barrier_semaphore()
    each(1, n, lambda t: pl.semaphore_signal(
        barrier, inc=1, device_id={"ctx": lax.rem(me + t, n)}, device_id_type=MESH))
    small = [pltpu.make_async_copy(starts_hbm, starts_ref, gsem.at[3]),
             pltpu.make_async_copy(mine_hbm, mine_ref, gsem.at[4])]
    for copy in small:
        copy.start()
    gate_copy = pltpu.make_async_copy(gate_hbm, gate_v, gsem.at[0])
    x_copy = pltpu.make_async_copy(x_hbm, x_ref, gsem.at[2])
    x_copy.start()
    gate_copy.start()
    for copy in small:
        copy.wait()
    lane = iota((1, LANES), 1)
    ordrow[...] = jnp.where(lane == 0, mine_ref[0], mine_ref[1])
    ordv[me] = jnp.where(lane == 0, mine_ref[0], mine_ref[1])

    bias, rate, skip = bias_ref[...], jnp.exp(decay_ref[...]), skip_ref[...]
    v = inc_ref[...].astype(F32).T + bias
    step = jnp.maximum(v, 0.0) + jnp.log(1.0 + jnp.exp(-jnp.abs(v)))
    fall = -step * rate
    tri = (iota((GROUP, GROUP), 0) >= iota((GROUP, GROUP), 1))
    ones = tri.astype(F32)
    logs, decs, tails = [], [], []
    keep0 = 1.0 - starts_ref[0].astype(F32)
    keep1 = 1.0 - starts_ref[1].astype(F32)
    for b in range(2):
        rows = slice(b * GROUP, (b + 1) * GROUP)
        st = step[rows, :]
        cum = jnp.dot(ones, fall[rows, :], preferred_element_type=F32, precision=lax.Precision.HIGHEST)
        end = cum[GROUP - 1:GROUP, :]
        decs.append((keep0, keep1)[b] * jnp.exp(end))
        tails.append(jnp.exp(end - cum) * st)
        exp_s[rows, :] = jnp.concatenate(split2(jnp.exp(cum)), axis=1)
        col_s[rows, :] = jnp.concatenate(split3(cum * LOG2E), axis=1)
        logs.append((jnp.log(st) - cum) * LOG2E)
        bt_s[rows, :] = b_ref[rows, :].astype(F32).T
    r16 = iota((16, HEAD_DIM), 0)
    small = jnp.where(r16 == 0, decs[0], jnp.where(r16 == 1, decs[1], jnp.where(r16 == 2, skip, 0.0)))
    tail_s[...] = jnp.concatenate(tails, axis=1).T
    exp_s[pl.ds(256, 16), :] = jnp.concatenate(split2(small), axis=1)

    left = iota((GROUP, LANES), 1) < HEAD_DIM
    x_copy.wait()

    def states_of(j):
        k = pair_at(j)
        lanes = lanes_of(k)
        pick = picks_two(k)
        ends = dot(exp_s[pl.ds(256, 16), :], pick)
        a0, a1 = ends[0:1, :], ends[1:2, :]
        states = []
        for b in range(2):
            rows = slice(b * GROUP, (b + 1) * GROUP)
            both = jnp.concatenate(
                [bt_s[rows, :] * tail_s[pl.ds(b * HEAD_DIM + 2 * k + e, 1), :] for e in range(2)], axis=0)
            out = dot(both.astype(BF16), x_ref[rows, lanes])
            states.append(jnp.where(left, out[:STATE], out[STATE:]))
        s0_s[j] = states[0]
        f_s[j] = (a1 * states[0] + states[1]).astype(BF16)
        d_s[j] = a0 * a1

    def swap(q):
        part = pl.ds(q * 8, 8)
        return (remote(f_s.at[part], pf.at[part], swf_s.at[q], swf_r.at[q], other),
                remote(d_s.at[part], pd.at[part], swd_s.at[q], swd_r.at[q], other))

    def begin(q):
        for copy in swap(q):
            copy.start()

    half = half_of(core)

    def join(j):
        mine, theirs = f_s[j, half, :].astype(F32), pf[j, half, :].astype(F32)
        dm, dt = d_s[j], pd[j]
        f0, f1 = jnp.where(first, mine, theirs), jnp.where(first, theirs, mine)
        fc[j] = (jnp.where(first, dt, dm) * f0 + f1).astype(BF16)
        dc[j] = dm * dt

    def quarter(h):
        return pl.ds(h * 32, 32)

    def send_state(j, h):
        to = 2 * pair_at(j) + core
        remote(fc.at[j, quarter(h)], rf.at[chip, quarter(h)], out_sem.at[0, h], out_sem.at[1, h], to).start()
        if h == 0:
            remote(dc.at[j], rd.at[chip], out_sem.at[0, 2], out_sem.at[1, 2], to).start()

    def join_chunk(q):
        for copy in swap(q):
            copy.wait_recv()
        each(q * 8, q * 8 + 8, join, 2)
        each(q * 8, min(q * 8 + 8, last), lambda j: send_state(j, 0))

    for q in range(4):
        each(q * 8, q * 8 + 8, states_of, 2)
        if q == 1:
            pl.semaphore_wait(barrier, n - 1)
            begin(0)
            begin(1)
        elif q > 1:
            join_chunk(q - 2)
            begin(q)
    join_chunk(2)
    each(1, n, lambda t: remote(
        ordrow, ordv.at[me], osem.at[0], osem.at[1], lax.rem(me + t, n)).start())
    row_s[...] = jnp.concatenate(logs, axis=1).T
    for b in range(2):
        rows = slice(b * GROUP, (b + 1) * GROUP)
        sc_s[rows, :] = lax.dot_general(
            c_ref[rows, :], b_ref[rows, :], (((1,), (1,)), ((), ())), preferred_element_type=F32)
    join_chunk(3)
    each(0, last, lambda j: send_state(j, 1))
    rf[chip] = fc[last]
    rd[chip] = dc[last]

    def local_of(j):
        k = pair_at(j)
        lanes = lanes_of(k)
        col = dot(col_s[...], picks_three(k))
        gain = dot(exp_s[pl.ds(256, 16), :], picks_two(k))[2:3, :]
        for b in range(2):
            rows = slice(b * GROUP, (b + 1) * GROUP)
            xb = x_ref[rows, lanes]
            outs = []
            for e in range(2):
                gap = col[rows, e * LANES:(e + 1) * LANES] + row_s[pl.ds(b * HEAD_DIM + 2 * k + e, 1), :]
                w = jnp.exp2(jnp.where(tri, gap, -1e30)) * sc_s[rows, :]
                outs.append(dot(w.astype(BF16), xb))
            m_s[j, rows, :] = jnp.where(left, outs[0], outs[1]) + gain * xb.astype(F32)

    def received(h):
        part = (pl.ds(0, last), quarter(h))
        remote(fc.at[part], rf.at[part], out_sem.at[0, h], out_sem.at[1, h], other).wait()

    def walk(h):
        def one(s, g):
            gs[s, quarter(h), :] = g.astype(BF16)
            return rd[s] * g + rf[s, quarter(h), :].astype(F32)

        lax.fori_loop(0, chips, one, jnp.zeros((32, LANES), F32))
        gh[core, last, quarter(h), :] = gs[chip, quarter(h), :]

    def send_back(i, h):
        s = shifted(i, 1)
        remote(gs.at[s, quarter(h)], gh.at[core, i, quarter(h)], back_s.at[h], back_r.at[h, i], 2 * s + core).start()

    each(0, W0, local_of, 2)
    remote(dc.at[pl.ds(0, last)], rd.at[pl.ds(0, last)], out_sem.at[0, 2], out_sem.at[1, 2], other).wait()
    received(0)
    walk(0)
    each(0, last, lambda t: send_back(last - 1 - t, 0))
    each(W0, W1, local_of, 2)
    received(1)
    walk(1)
    each(0, last, lambda t: send_back(last - 1 - t, 1))
    each(W1, chips, local_of, 2)
    gate_copy.wait()

    def arrived(i):
        for h in range(2):
            remote(gs.at[0, quarter(h)], gh.at[core, i, quarter(h)], back_s.at[h], back_r.at[h, i], other).wait_recv()

    def finish(i):
        k = pair_at(i)
        lanes = lanes_of(k)
        pick = picks_two(k)
        ex = dot(exp_s[...], pick)
        a0 = ex[256:257, :]
        g = jnp.concatenate([gh[0, i], gh[1, i]], axis=0).astype(F32)
        g = jnp.where(first, g, pd[i] * g + pf[i].astype(F32))
        after = a0 * g + s0_s[i]
        entering = ((keep0 * g).astype(BF16), (keep1 * after).astype(BF16))
        for b in range(2):
            rows = slice(b * GROUP, (b + 1) * GROUP)
            mixed = m_s[i, rows, :] + ex[rows, :] * dot(c_ref[rows, :], entering[b])
            z = gate_v[rows, lanes].astype(F32)
            st1[i, b] = (mixed * (z / (1.0 + jnp.exp(-z)))).astype(BF16)

    size = 64 // PARTS
    bufs = (buf0, buf1)

    def cut(c, p):
        return pl.ds(pl.multiple_of(c * 64 + p * size, size), size)

    def send_one(i, c, p):
        remote(st1.at[i, :, cut(c, p), :], bufs[p].at[pl.ds(2 * me, 2)],
               one_sem.at[0, p], one_sem.at[1, p], 2 * pair_at(i) + c).start()

    def send_last(p):
        remote(st1.at[last, :, cut(1 - core, p), :], bufs[p].at[pl.ds(2 * me, 2)],
               one_sem.at[0, p], one_sem.at[1, p], other).start()

    def finish_two(t):
        finish(2 * t + 1)
        finish(2 * t)
        for u in (3, 2):
            @pl.when(2 * t + u < last)
            def _():
                for c in range(2):
                    send_one(2 * t + u, c, 0)

    def swap_back(q):
        part = pl.ds(q * CHUNK, CHUNK)
        return remote(gh.at[core, part], gh.at[core, part], swg_s.at[q], swg_r.at[q], other)

    def swapped(q):
        part = pl.ds(q * CHUNK, CHUNK)
        return remote(gh.at[1 - core, part], gh.at[1 - core, part], swg_s.at[q], swg_r.at[q], other)

    rounds = chips // CHUNK
    for q in range(rounds - 1, -2, -1):
        if q >= 0:
            each(q * CHUNK, min(q * CHUNK + CHUNK, last), arrived)
            swap_back(q).start()
        if q < rounds - 1:
            swapped(q + 1).wait_recv()
            each(0, CHUNK // 2, lambda t: finish_two((q + 2) * CHUNK // 2 - 1 - t))
    for p in range(PARTS):
        bufs[p][pl.ds(2 * me, 2)] = st1[last, :, cut(core, p), :]
    for q in range(4):
        for copy in swap(q):
            copy.wait_send()
    for q in range(rounds):
        swap_back(q).wait_send()
    for h in range(2):
        part = (pl.ds(0, last), quarter(h))
        remote(gs.at[part], gs.at[part], back_s.at[h], back_r.at[h, 0], other).wait_send()
    for j in (1, 0):
        for c in range(2):
            send_one(j, c, 0)
    send_last(0)
    for p in range(1, PARTS):
        def rest(i):
            for c in range(2):
                send_one(i, c, p)

        each(0, last, rest)
        send_last(p)
    remote(ordv.at[pl.ds(0, n - 1)], ordv.at[pl.ds(0, n - 1)], osem.at[0], osem.at[1], other).wait()
    to_scalars = pltpu.make_async_copy(ordv, ordsm, gsem.at[1])
    to_scalars.start()
    to_scalars.wait()

    def send_two(i, p):
        remote(perm.at[p, i], out_ref.at[:, cut(core, p), lanes_of(chip)],
               two_sem.at[0, p], two_sem.at[1, p], device_at(i)).start()

    for p in range(PARTS):
        arrivals = remote(bufs[p].at[pl.ds(0, 2 * n - 2)], bufs[p].at[pl.ds(0, 2 * n - 2)],
                          one_sem.at[0, p], one_sem.at[1, p], other)
        arrivals.wait()

        def pick_and_send(i):
            to = device_at(i)
            for b in range(2):
                perm[p, i, b] = bufs[p][ordsm[to, 0, b]]

            @pl.when(i > 0)
            def _():
                send_two(i - 1, p)

        each(0, n - 1, pick_and_send)
        for b in range(2):
            out_ref[b, cut(core, p), lanes_of(chip)] = bufs[p][ordsm[me, 0, b]]
        send_two(n - 2, p)
    for p in range(PARTS):
        remote(perm.at[p, pl.ds(0, n - 1)], perm.at[p, pl.ds(0, n - 1)],
               two_sem.at[0, p], two_sem.at[1, p], other).wait()


def norm_kernel(v_ref, w_ref, o_hbm, o_v, osem):
    count = osem.shape[0]
    size = v_ref.shape[0] // count

    def rows(i):
        return pl.ds(pl.multiple_of(i * size, size), size)

    def store(i):
        return pltpu.make_async_copy(o_v.at[rows(i)], o_hbm.at[rows(i)], osem.at[i])

    def body(i):
        v = v_ref[rows(i), :].astype(F32)
        mean = jnp.mean(v * v, axis=-1, keepdims=True)
        o_v[rows(i), :] = (v * lax.rsqrt(mean + 1e-05) * w_ref[...]).astype(BF16)
        store(i).start()

    each(0, count, body)
    each(0, count, lambda i: store(i).wait())


def local(head_input, gate_input, write_vector, read_vector, increment_preactivation, step_bias,
          decay_log, skip_gain, norm_weight, doc_starts, block_order):
    n = lax.axis_size("ctx")
    chips = n // 2
    tokens, width = head_input.shape
    vmem = pl.BlockSpec(memory_space=pltpu.VMEM)
    hbm = pl.BlockSpec(memory_space=pltpu.HBM)
    dma = pltpu.SemaphoreType.DMA
    routed = pl.pallas_call(
        functools.partial(mega_kernel, n),
        out_shape=jax.ShapeDtypeStruct((2, GROUP, width), BF16),
        in_specs=[hbm] * 4 + [vmem] * 6,
        out_specs=vmem,
        scratch_shapes=[
            pltpu.SMEM((2,), jnp.int32),
            pltpu.SMEM((2,), jnp.int32),
            pltpu.VMEM((tokens, width), BF16),
            pltpu.VMEM((tokens, width), BF16),
            pltpu.VMEM((chips, tokens, LANES), F32),
            pltpu.VMEM((chips, STATE, LANES), F32),
            pltpu.VMEM((chips, STATE, LANES), BF16),
            pltpu.VMEM((chips, STATE, LANES), BF16),
            pltpu.VMEM((chips, 1, LANES), F32),
            pltpu.VMEM((chips, 1, LANES), F32),
            pltpu.VMEM((chips, 64, LANES), BF16),
            pltpu.VMEM((chips, 1, LANES), F32),
            pltpu.VMEM((chips, 64, LANES), BF16),
            pltpu.VMEM((chips, 1, LANES), F32),
            pltpu.VMEM((chips, 64, LANES), BF16),
            pltpu.VMEM((2, chips, 64, LANES), BF16),
            pltpu.VMEM((chips, 2, GROUP, LANES), BF16),
            pltpu.VMEM((2 * n, 64 // PARTS, LANES), BF16),
            pltpu.VMEM((2 * n, 64 // PARTS, LANES), BF16),
            pltpu.VMEM((PARTS, n, 2, 64 // PARTS, LANES), BF16),
            pltpu.VMEM((1, LANES), jnp.int32),
            pltpu.VMEM((n, 1, LANES), jnp.int32),
            pltpu.SMEM((n, 1, LANES), jnp.int32),
            pltpu.VMEM((2 * GROUP, 192), BF16),
            pltpu.VMEM((272, 2 * HEAD_DIM), BF16),
            pltpu.VMEM((2 * HEAD_DIM, GROUP), F32),
            pltpu.VMEM((2 * HEAD_DIM, GROUP), F32),
            pltpu.VMEM((2 * STATE, GROUP), F32),
            pltpu.VMEM((2 * GROUP, GROUP), F32),
            dma((5,)), dma((2,)), dma((4,)), dma((4,)), dma((4,)), dma((4,)), dma((2, 3)),
            dma((2,)), dma((2, chips)), dma((chips // CHUNK,)), dma((chips // CHUNK,)), dma((2, PARTS)), dma((2, PARTS)),
        ],
        compiler_params=pltpu.CompilerParams(
            collective_id=1, has_side_effects=True, vmem_limit_bytes=40 * 1024 * 1024),
        name="layer",
    )(*[pltpu.with_memory_space_constraint(v, pltpu.HBM) for v in (
        doc_starts, block_order, head_input, gate_input, write_vector, read_vector, increment_preactivation.T,
        step_bias[None], decay_log[None], skip_gain[None])])
    return pl.pallas_call(
        norm_kernel,
        out_shape=jax.ShapeDtypeStruct((tokens, width), BF16),
        in_specs=[vmem, vmem],
        out_specs=pl.BlockSpec(memory_space=pl.ANY),
        scratch_shapes=[pltpu.VMEM((tokens, width), BF16), dma((8,))],
        compiler_params=pltpu.CompilerParams(vmem_limit_bytes=8 * 1024 * 1024),
        name="gated_norm",
    )(routed.reshape(tokens, width), norm_weight[None])


def solution(mesh):
    return jax.shard_map(
        local,
        mesh=mesh,
        in_specs=(
            P(("dp", "ctx"), None),
            P(("dp", "ctx"), None),
            P(("dp", "ctx"), None),
            P(("dp", "ctx"), None),
            P(("dp", "ctx"), None),
            P(),
            P(),
            P(),
            P(),
            P(("dp", "ctx")),
            P(("dp", "ctx")),
        ),
        out_specs=P(("dp", "ctx"), None),
        check_vma=False,
    )
```

```python
import functools

import jax
import jax.numpy as jnp
from jax import lax
from jax.experimental import pallas as pl
from jax.experimental.pallas import tpu as pltpu
from jax.sharding import PartitionSpec as P

GROUP = 128
HEAD_DIM = 64
STATE = 128
LANES = 128
LOG2E = 1.4426950408889634
F32 = jnp.float32
BF16 = jnp.bfloat16
MESH = pl.DeviceIdType.MESH


def high(v):
    return v.astype(BF16).astype(F32)


def split2(v):
    hi = high(v)
    return hi.astype(BF16), (v - hi).astype(BF16)


def split3(v):
    hi = high(v)
    mid = high(v - hi)
    return hi.astype(BF16), mid.astype(BF16), (v - hi - mid).astype(BF16)


def dot(a, b):
    return jnp.dot(a, b, preferred_element_type=F32)


def iota(shape, dim):
    return lax.broadcasted_iota(jnp.int32, shape, dim)


def picks_two(k):
    shape = (2 * HEAD_DIM, LANES)
    return ((iota(shape, 0) & 63) == 2 * k + (iota(shape, 1) >> 6)).astype(BF16)


def picks_three(k):
    shape = (192, 2 * LANES)
    return ((iota(shape, 0) & 63) == 2 * k + (iota(shape, 1) >> 7)).astype(BF16)


def remote(src, dst, send, recv, device):
    return pltpu.make_async_remote_copy(
        src_ref=src, dst_ref=dst, send_sem=send, recv_sem=recv,
        device_id={"ctx": device}, device_id_type=MESH)


def around(i, n):
    return jnp.where(i == n - 1, 0, jnp.where((i & 1) == 0, i // 2 + 1, n - (i + 1) // 2))


def each(lo, hi, act, step=1):
    def body(i, carry):
        for u in range(step):
            act(lo + i * step + u)
        return carry

    lax.fori_loop(0, (hi - lo) // step, body, 0)


PARTS = 2
W0, W1 = 12, 22
CHUNK = 2


def mega_kernel(n, starts_hbm, mine_hbm, x_hbm, gate_hbm, b_hbm, c_hbm, inc_hbm, bias_hbm, decay_hbm, skip_hbm, out_ref,
                starts_ref, mine_ref, b_ref, c_ref, inc_ref, bias_ref, decay_ref, skip_ref, cum_s, step_s, x_ref, gate_v, m_s, s0_s, f_s, pf, d_s, pd, fc, dc, rf, rd, gs, gh, st1, buf0, buf1, perm,
                ordrow, ordv, ordsm, col_s, exp_s, row_s, tail_s, bt_s, sc_s,
                gsem, osem, swf_s, swf_r, swd_s, swd_r, out_sem, back_s, back_r, swg_s, swg_r, one_sem, two_sem):
    me = lax.axis_index("ctx")
    chip, core = me // 2, me % 2
    chips = n // 2
    last = chips - 1
    other = chip * 2 + (1 - core)
    first = core == 0

    def shifted(j, sign):
        return lax.rem(chip + sign * around(j, chips) + chips, chips)

    def pair_at(j):
        return shifted(j, -1)

    def device_at(i):
        return lax.rem(me + around(i, n), n)

    def lanes_of(k):
        return pl.ds(pl.multiple_of(k * LANES, LANES), LANES)

    def half_of(c):
        return pl.ds(pl.multiple_of(c * 64, 64), 64)

    loads = [pltpu.make_async_copy(src, dst, gsem.at[i]) for i, (src, dst) in enumerate((
        (inc_hbm, inc_ref), (bias_hbm, bias_ref), (decay_hbm, decay_ref), (b_hbm, b_ref), (starts_hbm, starts_ref),
        (skip_hbm, skip_ref), (x_hbm, x_ref), (mine_hbm, mine_ref), (c_hbm, c_ref), (gate_hbm, gate_v)))]
    for copy in loads[:3]:
        copy.start()
    barrier = pltpu.get_barrier_semaphore()
    each(1, n, lambda t: pl.semaphore_signal(
        barrier, inc=1, device_id={"ctx": lax.rem(me + t, n)}, device_id_type=MESH))
    for copy in loads[3:]:
        copy.start()

    tri = (iota((GROUP, GROUP), 0) >= iota((GROUP, GROUP), 1))
    ones = tri.astype(F32)
    for copy in loads[:3]:
        copy.wait()
    v = inc_ref[...].astype(F32).T + bias_ref[...]
    step = jnp.maximum(v, 0.0) + jnp.log(1.0 + jnp.exp(-jnp.abs(v)))
    step_s[...] = step
    fall = -step * jnp.exp(decay_ref[...])
    ends, tails = [], []
    for b in range(2):
        rows = slice(b * GROUP, (b + 1) * GROUP)
        cum = jnp.dot(ones, fall[rows, :], preferred_element_type=F32, precision=lax.Precision.HIGHEST)
        cum_s[rows, :] = cum
        ends.append(cum[GROUP - 1:GROUP, :])
        tails.append(jnp.exp(ends[b] - cum) * step[rows, :])
    tail_s[...] = jnp.concatenate(tails, axis=1).T
    for copy in loads[3:6]:
        copy.wait()
    keep0 = 1.0 - starts_ref[0].astype(F32)
    keep1 = 1.0 - starts_ref[1].astype(F32)
    for b in range(2):
        rows = slice(b * GROUP, (b + 1) * GROUP)
        bt_s[rows, :] = b_ref[rows, :].astype(F32).T
    r16 = iota((16, HEAD_DIM), 0)
    small = jnp.where(r16 == 0, keep0 * jnp.exp(ends[0]), jnp.where(
        r16 == 1, keep1 * jnp.exp(ends[1]), jnp.where(r16 == 2, skip_ref[...], 0.0)))
    exp_s[pl.ds(256, 16), :] = jnp.concatenate(split2(small), axis=1)
    loads[7].wait()
    lane = iota((1, LANES), 1)
    ordrow[...] = jnp.where(lane == 0, mine_ref[0], mine_ref[1])
    ordv[me] = jnp.where(lane == 0, mine_ref[0], mine_ref[1])

    left = iota((GROUP, LANES), 1) < HEAD_DIM
    loads[6].wait()

    def states_of(j):
        k = pair_at(j)
        lanes = lanes_of(k)
        pick = picks_two(k)
        ends = dot(exp_s[pl.ds(256, 16), :], pick)
        a0, a1 = ends[0:1, :], ends[1:2, :]
        states = []
        for b in range(2):
            rows = slice(b * GROUP, (b + 1) * GROUP)
            both = jnp.concatenate(
                [bt_s[rows, :] * tail_s[pl.ds(b * HEAD_DIM + 2 * k + e, 1), :] for e in range(2)], axis=0)
            out = dot(both.astype(BF16), x_ref[rows, lanes])
            states.append(jnp.where(left, out[:STATE], out[STATE:]))
        s0_s[j] = states[0]
        f_s[j] = (a1 * states[0] + states[1]).astype(BF16)
        d_s[j] = a0 * a1

    def swap(q):
        part = pl.ds(q * 8, 8)
        return (remote(f_s.at[part], pf.at[part], swf_s.at[q], swf_r.at[q], other),
                remote(d_s.at[part], pd.at[part], swd_s.at[q], swd_r.at[q], other))

    def begin(q):
        for copy in swap(q):
            copy.start()

    half = half_of(core)

    def join(j):
        mine, theirs = f_s[j, half, :].astype(F32), pf[j, half, :].astype(F32)
        dm, dt = d_s[j], pd[j]
        f0, f1 = jnp.where(first, mine, theirs), jnp.where(first, theirs, mine)
        fc[j] = (jnp.where(first, dt, dm) * f0 + f1).astype(BF16)
        dc[j] = dm * dt

    def quarter(h):
        return pl.ds(h * 32, 32)

    def send_state(j, h):
        to = 2 * pair_at(j) + core
        remote(fc.at[j, quarter(h)], rf.at[chip, quarter(h)], out_sem.at[0, h], out_sem.at[1, h], to).start()
        if h == 0:
            remote(dc.at[j], rd.at[chip], out_sem.at[0, 2], out_sem.at[1, 2], to).start()

    def join_chunk(q):
        for copy in swap(q):
            copy.wait_recv()
        each(q * 8, q * 8 + 8, join, 2)
        each(q * 8, min(q * 8 + 8, last), lambda j: send_state(j, 0))

    for q in range(4):
        each(q * 8, q * 8 + 8, states_of, 2)
        if q == 1:
            pl.semaphore_wait(barrier, n - 1)
            begin(0)
            begin(1)
            each(1, n, lambda t: remote(
                ordrow, ordv.at[me], osem.at[0], osem.at[1], lax.rem(me + t, n)).start())
        elif q > 1:
            join_chunk(q - 2)
            begin(q)
    join_chunk(2)
    loads[8].wait()
    logs = []
    for b in range(2):
        rows = slice(b * GROUP, (b + 1) * GROUP)
        cum = cum_s[rows, :]
        exp_s[rows, :] = jnp.concatenate(split2(jnp.exp(cum)), axis=1)
        col_s[rows, :] = jnp.concatenate(split3(cum * LOG2E), axis=1)
        logs.append((jnp.log(step_s[rows, :]) - cum) * LOG2E)
        sc_s[rows, :] = lax.dot_general(
            c_ref[rows, :], b_ref[rows, :], (((1,), (1,)), ((), ())), preferred_element_type=F32)
    row_s[...] = jnp.concatenate(logs, axis=1).T
    join_chunk(3)
    each(0, last, lambda j: send_state(j, 1))
    rf[chip] = fc[last]
    rd[chip] = dc[last]

    def local_of(j):
        k = pair_at(j)
        lanes = lanes_of(k)
        col = dot(col_s[...], picks_three(k))
        gain = dot(exp_s[pl.ds(256, 16), :], picks_two(k))[2:3, :]
        for b in range(2):
            rows = slice(b * GROUP, (b + 1) * GROUP)
            xb = x_ref[rows, lanes]
            outs = []
            for e in range(2):
                gap = col[rows, e * LANES:(e + 1) * LANES] + row_s[pl.ds(b * HEAD_DIM + 2 * k + e, 1), :]
                w = jnp.exp2(jnp.where(tri, gap, -1e30)) * sc_s[rows, :]
                outs.append(dot(w.astype(BF16), xb))
            m_s[j, rows, :] = jnp.where(left, outs[0], outs[1]) + gain * xb.astype(F32)

    def received(h):
        part = (pl.ds(0, last), quarter(h))
        remote(fc.at[part], rf.at[part], out_sem.at[0, h], out_sem.at[1, h], other).wait()

    def walk(h):
        def one(s, g):
            gs[s, quarter(h), :] = g.astype(BF16)
            return rd[s] * g + rf[s, quarter(h), :].astype(F32)

        lax.fori_loop(0, chips, one, jnp.zeros((32, LANES), F32))
        gh[core, last, quarter(h), :] = gs[chip, quarter(h), :]

    def send_back(i, h):
        s = shifted(i, 1)
        remote(gs.at[s, quarter(h)], gh.at[core, i, quarter(h)], back_s.at[h], back_r.at[h, i], 2 * s + core).start()

    each(0, W0, local_of, 2)
    remote(dc.at[pl.ds(0, last)], rd.at[pl.ds(0, last)], out_sem.at[0, 2], out_sem.at[1, 2], other).wait()
    received(0)
    walk(0)
    each(0, last, lambda t: send_back(last - 1 - t, 0))
    each(W0, W1, local_of, 2)
    received(1)
    walk(1)
    each(0, last, lambda t: send_back(last - 1 - t, 1))
    each(W1, chips, local_of, 2)
    loads[9].wait()

    def arrived(i):
        for h in range(2):
            remote(gs.at[0, quarter(h)], gh.at[core, i, quarter(h)], back_s.at[h], back_r.at[h, i], other).wait_recv()

    def finish(i):
        k = pair_at(i)
        lanes = lanes_of(k)
        pick = picks_two(k)
        ex = dot(exp_s[...], pick)
        a0 = ex[256:257, :]
        g = jnp.concatenate([gh[0, i], gh[1, i]], axis=0).astype(F32)
        g = jnp.where(first, g, pd[i] * g + pf[i].astype(F32))
        after = a0 * g + s0_s[i]
        entering = ((keep0 * g).astype(BF16), (keep1 * after).astype(BF16))
        for b in range(2):
            rows = slice(b * GROUP, (b + 1) * GROUP)
            mixed = m_s[i, rows, :] + ex[rows, :] * dot(c_ref[rows, :], entering[b])
            z = gate_v[rows, lanes].astype(F32)
            st1[i, b] = (mixed * (z / (1.0 + jnp.exp(-z)))).astype(BF16)

    size = 64 // PARTS
    bufs = (buf0, buf1)

    def cut(c, p):
        return pl.ds(pl.multiple_of(c * 64 + p * size, size), size)

    def send_one(i, c, p):
        remote(st1.at[i, :, cut(c, p), :], bufs[p].at[pl.ds(2 * me, 2)],
               one_sem.at[0, p], one_sem.at[1, p], 2 * pair_at(i) + c).start()

    def send_last(p):
        remote(st1.at[last, :, cut(1 - core, p), :], bufs[p].at[pl.ds(2 * me, 2)],
               one_sem.at[0, p], one_sem.at[1, p], other).start()

    def finish_two(t):
        finish(2 * t + 1)
        finish(2 * t)
        for u in (3, 2):
            @pl.when(2 * t + u < last)
            def _():
                for c in range(2):
                    send_one(2 * t + u, c, 0)

    def swap_back(q):
        part = pl.ds(q * CHUNK, CHUNK)
        return remote(gh.at[core, part], gh.at[core, part], swg_s.at[q], swg_r.at[q], other)

    def swapped(q):
        part = pl.ds(q * CHUNK, CHUNK)
        return remote(gh.at[1 - core, part], gh.at[1 - core, part], swg_s.at[q], swg_r.at[q], other)

    rounds = chips // CHUNK
    for q in range(rounds - 1, -2, -1):
        if q >= 0:
            each(q * CHUNK, min(q * CHUNK + CHUNK, last), arrived)
            swap_back(q).start()
        if q < rounds - 1:
            swapped(q + 1).wait_recv()
            each(0, CHUNK // 2, lambda t: finish_two((q + 2) * CHUNK // 2 - 1 - t))
    for p in range(PARTS):
        bufs[p][pl.ds(2 * me, 2)] = st1[last, :, cut(core, p), :]
    for q in range(4):
        for copy in swap(q):
            copy.wait_send()
    for q in range(rounds):
        swap_back(q).wait_send()
    for h in range(2):
        part = (pl.ds(0, last), quarter(h))
        remote(gs.at[part], gs.at[part], back_s.at[h], back_r.at[h, 0], other).wait_send()
    for j in (1, 0):
        for c in range(2):
            send_one(j, c, 0)
    send_last(0)
    for p in range(1, PARTS):
        def rest(i):
            for c in range(2):
                send_one(i, c, p)

        each(0, last, rest)
        send_last(p)
    remote(ordv.at[pl.ds(0, n - 1)], ordv.at[pl.ds(0, n - 1)], osem.at[0], osem.at[1], other).wait()
    to_scalars = pltpu.make_async_copy(ordv, ordsm, gsem.at[10])
    to_scalars.start()
    to_scalars.wait()

    def send_two(i, p):
        remote(perm.at[p, i], out_ref.at[:, cut(core, p), lanes_of(chip)],
               two_sem.at[0, p], two_sem.at[1, p], device_at(i)).start()

    for p in range(PARTS):
        arrivals = remote(bufs[p].at[pl.ds(0, 2 * n - 2)], bufs[p].at[pl.ds(0, 2 * n - 2)],
                          one_sem.at[0, p], one_sem.at[1, p], other)
        arrivals.wait()

        def pick_and_send(i):
            to = device_at(i)
            for b in range(2):
                perm[p, i, b] = bufs[p][ordsm[to, 0, b]]

            @pl.when(i > 0)
            def _():
                send_two(i - 1, p)

        each(0, n - 1, pick_and_send)
        for b in range(2):
            out_ref[b, cut(core, p), lanes_of(chip)] = bufs[p][ordsm[me, 0, b]]
        send_two(n - 2, p)
    for p in range(PARTS):
        remote(perm.at[p, pl.ds(0, n - 1)], perm.at[p, pl.ds(0, n - 1)],
               two_sem.at[0, p], two_sem.at[1, p], other).wait()


def norm_kernel(v_ref, w_ref, o_hbm, o_v, osem):
    count = osem.shape[0]
    size = v_ref.shape[0] // count

    def rows(i):
        return pl.ds(pl.multiple_of(i * size, size), size)

    def store(i):
        return pltpu.make_async_copy(o_v.at[rows(i)], o_hbm.at[rows(i)], osem.at[i])

    def body(i):
        v = v_ref[rows(i), :].astype(F32)
        mean = jnp.mean(v * v, axis=-1, keepdims=True)
        o_v[rows(i), :] = (v * lax.rsqrt(mean + 1e-05) * w_ref[...]).astype(BF16)
        store(i).start()

    each(0, count, body)
    each(0, count, lambda i: store(i).wait())


def local(head_input, gate_input, write_vector, read_vector, increment_preactivation, step_bias,
          decay_log, skip_gain, norm_weight, doc_starts, block_order):
    n = lax.axis_size("ctx")
    chips = n // 2
    tokens, width = head_input.shape
    vmem = pl.BlockSpec(memory_space=pltpu.VMEM)
    hbm = pl.BlockSpec(memory_space=pltpu.HBM)
    dma = pltpu.SemaphoreType.DMA
    routed = pl.pallas_call(
        functools.partial(mega_kernel, n),
        out_shape=jax.ShapeDtypeStruct((2, GROUP, width), BF16),
        in_specs=[hbm] * 10,
        out_specs=vmem,
        scratch_shapes=[
            pltpu.SMEM((2,), jnp.int32),
            pltpu.SMEM((2,), jnp.int32),
            pltpu.VMEM((tokens, STATE), BF16),
            pltpu.VMEM((tokens, STATE), BF16),
            pltpu.VMEM((HEAD_DIM, tokens), BF16),
            pltpu.VMEM((1, HEAD_DIM), F32),
            pltpu.VMEM((1, HEAD_DIM), F32),
            pltpu.VMEM((1, HEAD_DIM), F32),
            pltpu.VMEM((tokens, HEAD_DIM), F32),
            pltpu.VMEM((tokens, HEAD_DIM), F32),
            pltpu.VMEM((tokens, width), BF16),
            pltpu.VMEM((tokens, width), BF16),
            pltpu.VMEM((chips, tokens, LANES), F32),
            pltpu.VMEM((chips, STATE, LANES), F32),
            pltpu.VMEM((chips, STATE, LANES), BF16),
            pltpu.VMEM((chips, STATE, LANES), BF16),
            pltpu.VMEM((chips, 1, LANES), F32),
            pltpu.VMEM((chips, 1, LANES), F32),
            pltpu.VMEM((chips, 64, LANES), BF16),
            pltpu.VMEM((chips, 1, LANES), F32),
            pltpu.VMEM((chips, 64, LANES), BF16),
            pltpu.VMEM((chips, 1, LANES), F32),
            pltpu.VMEM((chips, 64, LANES), BF16),
            pltpu.VMEM((2, chips, 64, LANES), BF16),
            pltpu.VMEM((chips, 2, GROUP, LANES), BF16),
            pltpu.VMEM((2 * n, 64 // PARTS, LANES), BF16),
            pltpu.VMEM((2 * n, 64 // PARTS, LANES), BF16),
            pltpu.VMEM((PARTS, n, 2, 64 // PARTS, LANES), BF16),
            pltpu.VMEM((1, LANES), jnp.int32),
            pltpu.VMEM((n, 1, LANES), jnp.int32),
            pltpu.SMEM((n, 1, LANES), jnp.int32),
            pltpu.VMEM((2 * GROUP, 192), BF16),
            pltpu.VMEM((272, 2 * HEAD_DIM), BF16),
            pltpu.VMEM((2 * HEAD_DIM, GROUP), F32),
            pltpu.VMEM((2 * HEAD_DIM, GROUP), F32),
            pltpu.VMEM((2 * STATE, GROUP), F32),
            pltpu.VMEM((2 * GROUP, GROUP), F32),
            dma((11,)), dma((2,)), dma((4,)), dma((4,)), dma((4,)), dma((4,)), dma((2, 3)),
            dma((2,)), dma((2, chips)), dma((chips // CHUNK,)), dma((chips // CHUNK,)), dma((2, PARTS)), dma((2, PARTS)),
        ],
        compiler_params=pltpu.CompilerParams(
            collective_id=1, has_side_effects=True, vmem_limit_bytes=40 * 1024 * 1024),
        name="layer",
    )(*[pltpu.with_memory_space_constraint(v, pltpu.HBM) for v in (
        doc_starts, block_order, head_input, gate_input, write_vector, read_vector, increment_preactivation.T,
        step_bias[None], decay_log[None], skip_gain[None])])
    return pl.pallas_call(
        norm_kernel,
        out_shape=jax.ShapeDtypeStruct((tokens, width), BF16),
        in_specs=[vmem, vmem],
        out_specs=pl.BlockSpec(memory_space=pl.ANY),
        scratch_shapes=[pltpu.VMEM((tokens, width), BF16), dma((8,))],
        compiler_params=pltpu.CompilerParams(vmem_limit_bytes=8 * 1024 * 1024),
        name="gated_norm",
    )(routed.reshape(tokens, width), norm_weight[None])


def solution(mesh):
    return jax.shard_map(
        local,
        mesh=mesh,
        in_specs=(
            P(("dp", "ctx"), None),
            P(("dp", "ctx"), None),
            P(("dp", "ctx"), None),
            P(("dp", "ctx"), None),
            P(("dp", "ctx"), None),
            P(),
            P(),
            P(),
            P(),
            P(("dp", "ctx")),
            P(("dp", "ctx")),
        ),
        out_specs=P(("dp", "ctx"), None),
        check_vma=False,
    )
```

```python
import functools

import jax
import jax.numpy as jnp
from jax import lax
from jax.experimental import pallas as pl
from jax.experimental.pallas import tpu as pltpu
from jax.sharding import PartitionSpec as P

GROUP = 128
HEAD_DIM = 64
STATE = 128
LANES = 128
LOG2E = 1.4426950408889634
F32 = jnp.float32
BF16 = jnp.bfloat16
MESH = pl.DeviceIdType.MESH


def high(v):
    return v.astype(BF16).astype(F32)


def split2(v):
    hi = high(v)
    return hi.astype(BF16), (v - hi).astype(BF16)


def split3(v):
    hi = high(v)
    mid = high(v - hi)
    return hi.astype(BF16), mid.astype(BF16), (v - hi - mid).astype(BF16)


def dot(a, b):
    return jnp.dot(a, b, preferred_element_type=F32)


def iota(shape, dim):
    return lax.broadcasted_iota(jnp.int32, shape, dim)


def picks_two(k):
    shape = (2 * HEAD_DIM, LANES)
    return ((iota(shape, 0) & 63) == 2 * k + (iota(shape, 1) >> 6)).astype(BF16)


def picks_three(k):
    shape = (192, 2 * LANES)
    return ((iota(shape, 0) & 63) == 2 * k + (iota(shape, 1) >> 7)).astype(BF16)


def remote(src, dst, send, recv, device):
    return pltpu.make_async_remote_copy(
        src_ref=src, dst_ref=dst, send_sem=send, recv_sem=recv,
        device_id={"ctx": device}, device_id_type=MESH)


def around(i, n):
    return jnp.where(i == n - 1, 0, jnp.where((i & 1) == 0, i // 2 + 1, n - (i + 1) // 2))


def each(lo, hi, act, step=1):
    def body(i, carry):
        for u in range(step):
            act(lo + i * step + u)
        return carry

    lax.fori_loop(0, (hi - lo) // step, body, 0)


SPLIT = (32, 32)
PARTS = len(SPLIT)
W0, W1 = 12, 22
CHUNK = 2


def mega_kernel(n, starts_hbm, mine_hbm, x_hbm, gate_hbm, b_hbm, c_hbm, inc_hbm, bias_hbm, decay_hbm, skip_hbm, gain_hbm, out_ref,
                starts_ref, mine_ref, b_ref, c_ref, inc_ref, bias_ref, decay_ref, skip_ref, gain_ref, cum_s, step_s, x_ref, gate_v, m_s, s0_s, f_s, pf, d_s, pd, fc, dc, rf, rd, gs, gh, st1, buf0, buf1, perm0, perm1,
                ordrow, ordv, ordsm, col_s, exp_s, row_s, tail_s, bt_s, sc_s,
                gsem, osem, swf_s, swf_r, swd_s, swd_r, out_sem, back_s, back_r, swg_s, swg_r, one_sem, two_sem):
    me = lax.axis_index("ctx")
    chip, core = me // 2, me % 2
    chips = n // 2
    last = chips - 1
    other = chip * 2 + (1 - core)
    first = core == 0

    def shifted(j, sign):
        return lax.rem(chip + sign * around(j, chips) + chips, chips)

    def pair_at(j):
        return shifted(j, -1)

    def device_at(i):
        return lax.rem(me + around(i, n), n)

    def lanes_of(k):
        return pl.ds(pl.multiple_of(k * LANES, LANES), LANES)

    def half_of(c):
        return pl.ds(pl.multiple_of(c * 64, 64), 64)

    loads = [pltpu.make_async_copy(src, dst, gsem.at[i]) for i, (src, dst) in enumerate((
        (inc_hbm, inc_ref), (bias_hbm, bias_ref), (decay_hbm, decay_ref), (b_hbm, b_ref), (starts_hbm, starts_ref),
        (skip_hbm, skip_ref), (x_hbm, x_ref), (mine_hbm, mine_ref), (c_hbm, c_ref), (gate_hbm, gate_v), (gain_hbm, gain_ref)))]
    for copy in loads[:3]:
        copy.start()
    barrier = pltpu.get_barrier_semaphore()
    each(1, n, lambda t: pl.semaphore_signal(
        barrier, inc=1, device_id={"ctx": lax.rem(me + t, n)}, device_id_type=MESH))
    for copy in loads[3:]:
        copy.start()

    tri = (iota((GROUP, GROUP), 0) >= iota((GROUP, GROUP), 1))
    ones = tri.astype(F32)
    for copy in loads[:3]:
        copy.wait()
    v = inc_ref[...].astype(F32).T + bias_ref[...]
    step = jnp.maximum(v, 0.0) + jnp.log(1.0 + jnp.exp(-jnp.abs(v)))
    step_s[...] = step
    fall = -step * jnp.exp(decay_ref[...])
    ends, tails = [], []
    for b in range(2):
        rows = slice(b * GROUP, (b + 1) * GROUP)
        cum = jnp.dot(ones, fall[rows, :], preferred_element_type=F32, precision=lax.Precision.HIGHEST)
        cum_s[rows, :] = cum
        ends.append(cum[GROUP - 1:GROUP, :])
        tails.append(jnp.exp(ends[b] - cum) * step[rows, :])
    tail_s[...] = jnp.concatenate(tails, axis=1).T
    for copy in loads[3:6]:
        copy.wait()
    keep0 = 1.0 - starts_ref[0].astype(F32)
    keep1 = 1.0 - starts_ref[1].astype(F32)
    for b in range(2):
        rows = slice(b * GROUP, (b + 1) * GROUP)
        bt_s[rows, :] = b_ref[rows, :].astype(F32).T
    r16 = iota((16, HEAD_DIM), 0)
    small = jnp.where(r16 == 0, keep0 * jnp.exp(ends[0]), jnp.where(
        r16 == 1, keep1 * jnp.exp(ends[1]), jnp.where(r16 == 2, skip_ref[...], 0.0)))
    exp_s[pl.ds(256, 16), :] = jnp.concatenate(split2(small), axis=1)
    loads[7].wait()
    lane = iota((1, LANES), 1)
    ordrow[...] = jnp.where(lane == 0, mine_ref[0], mine_ref[1])
    ordv[me] = jnp.where(lane == 0, mine_ref[0], mine_ref[1])

    left = iota((GROUP, LANES), 1) < HEAD_DIM
    loads[6].wait()

    def states_of(j):
        k = pair_at(j)
        lanes = lanes_of(k)
        pick = picks_two(k)
        ends = dot(exp_s[pl.ds(256, 16), :], pick)
        a0, a1 = ends[0:1, :], ends[1:2, :]
        states = []
        for b in range(2):
            rows = slice(b * GROUP, (b + 1) * GROUP)
            both = jnp.concatenate(
                [bt_s[rows, :] * tail_s[pl.ds(b * HEAD_DIM + 2 * k + e, 1), :] for e in range(2)], axis=0)
            out = dot(both.astype(BF16), x_ref[rows, lanes])
            states.append(jnp.where(left, out[:STATE], out[STATE:]))
        s0_s[j] = states[0]
        f_s[j] = (a1 * states[0] + states[1]).astype(BF16)
        d_s[j] = a0 * a1

    def swap(q):
        part = pl.ds(q * 8, 8)
        return (remote(f_s.at[part], pf.at[part], swf_s.at[q], swf_r.at[q], other),
                remote(d_s.at[part], pd.at[part], swd_s.at[q], swd_r.at[q], other))

    def begin(q):
        for copy in swap(q):
            copy.start()

    half = half_of(core)

    def join(j):
        mine, theirs = f_s[j, half, :].astype(F32), pf[j, half, :].astype(F32)
        dm, dt = d_s[j], pd[j]
        f0, f1 = jnp.where(first, mine, theirs), jnp.where(first, theirs, mine)
        fc[j] = (jnp.where(first, dt, dm) * f0 + f1).astype(BF16)
        dc[j] = dm * dt

    def quarter(h):
        return pl.ds(h * 32, 32)

    def send_state(j, h):
        to = 2 * pair_at(j) + core
        remote(fc.at[j, quarter(h)], rf.at[chip, quarter(h)], out_sem.at[0, h], out_sem.at[1, h], to).start()
        if h == 0:
            remote(dc.at[j], rd.at[chip], out_sem.at[0, 2], out_sem.at[1, 2], to).start()

    def join_chunk(q):
        for copy in swap(q):
            copy.wait_recv()
        each(q * 8, q * 8 + 8, join, 2)
        each(q * 8, min(q * 8 + 8, last), lambda j: send_state(j, 0))

    for q in range(4):
        each(q * 8, q * 8 + 8, states_of, 2)
        if q == 1:
            pl.semaphore_wait(barrier, n - 1)
            begin(0)
            begin(1)
            each(1, n, lambda t: remote(
                ordrow, ordv.at[me], osem.at[0], osem.at[1], lax.rem(me + t, n)).start())
        elif q > 1:
            join_chunk(q - 2)
            begin(q)
    join_chunk(2)
    loads[8].wait()
    logs = []
    for b in range(2):
        rows = slice(b * GROUP, (b + 1) * GROUP)
        cum = cum_s[rows, :]
        exp_s[rows, :] = jnp.concatenate(split2(jnp.exp(cum)), axis=1)
        col_s[rows, :] = jnp.concatenate(split3(cum * LOG2E), axis=1)
        logs.append((jnp.log(step_s[rows, :]) - cum) * LOG2E)
        sc_s[rows, :] = lax.dot_general(
            c_ref[rows, :], b_ref[rows, :], (((1,), (1,)), ((), ())), preferred_element_type=F32)
    row_s[...] = jnp.concatenate(logs, axis=1).T
    join_chunk(3)
    each(0, last, lambda j: send_state(j, 1))
    rf[chip] = fc[last]
    rd[chip] = dc[last]

    def local_of(j):
        k = pair_at(j)
        lanes = lanes_of(k)
        col = dot(col_s[...], picks_three(k))
        gain = dot(exp_s[pl.ds(256, 16), :], picks_two(k))[2:3, :]
        for b in range(2):
            rows = slice(b * GROUP, (b + 1) * GROUP)
            xb = x_ref[rows, lanes]
            outs = []
            for e in range(2):
                gap = col[rows, e * LANES:(e + 1) * LANES] + row_s[pl.ds(b * HEAD_DIM + 2 * k + e, 1), :]
                w = jnp.exp2(jnp.where(tri, gap, -1e30)) * sc_s[rows, :]
                outs.append(dot(w.astype(BF16), xb))
            m_s[j, rows, :] = jnp.where(left, outs[0], outs[1]) + gain * xb.astype(F32)

    def received(h):
        part = (pl.ds(0, last), quarter(h))
        remote(fc.at[part], rf.at[part], out_sem.at[0, h], out_sem.at[1, h], other).wait()

    def walk(h):
        def one(s, g):
            gs[s, quarter(h), :] = g.astype(BF16)
            return rd[s] * g + rf[s, quarter(h), :].astype(F32)

        lax.fori_loop(0, chips, one, jnp.zeros((32, LANES), F32))
        gh[core, last, quarter(h), :] = gs[chip, quarter(h), :]

    def send_back(i, h):
        s = shifted(i, 1)
        remote(gs.at[s, quarter(h)], gh.at[core, i, quarter(h)], back_s.at[h], back_r.at[h, i], 2 * s + core).start()

    each(0, W0, local_of, 2)
    remote(dc.at[pl.ds(0, last)], rd.at[pl.ds(0, last)], out_sem.at[0, 2], out_sem.at[1, 2], other).wait()
    received(0)
    walk(0)
    each(0, last, lambda t: send_back(last - 1 - t, 0))
    each(W0, W1, local_of, 2)
    received(1)
    walk(1)
    each(0, last, lambda t: send_back(last - 1 - t, 1))
    each(W1, chips, local_of, 2)
    loads[9].wait()

    def arrived(i):
        for h in range(2):
            remote(gs.at[0, quarter(h)], gh.at[core, i, quarter(h)], back_s.at[h], back_r.at[h, i], other).wait_recv()

    def finish(i):
        k = pair_at(i)
        lanes = lanes_of(k)
        pick = picks_two(k)
        ex = dot(exp_s[...], pick)
        a0 = ex[256:257, :]
        g = jnp.concatenate([gh[0, i], gh[1, i]], axis=0).astype(F32)
        g = jnp.where(first, g, pd[i] * g + pf[i].astype(F32))
        after = a0 * g + s0_s[i]
        entering = ((keep0 * g).astype(BF16), (keep1 * after).astype(BF16))
        for b in range(2):
            rows = slice(b * GROUP, (b + 1) * GROUP)
            mixed = m_s[i, rows, :] + ex[rows, :] * dot(c_ref[rows, :], entering[b])
            z = gate_v[rows, lanes].astype(F32)
            st1[i, b] = (mixed * (z / (1.0 + jnp.exp(-z)))).astype(BF16)

    bufs, perms = (buf0, buf1), (perm0, perm1)

    def cut(c, p):
        return pl.ds(pl.multiple_of(c * 64 + sum(SPLIT[:p]), 16), SPLIT[p])

    def send_one(i, c, p):
        remote(st1.at[i, :, cut(c, p), :], bufs[p].at[pl.ds(2 * me, 2)],
               one_sem.at[0, p], one_sem.at[1, p], 2 * pair_at(i) + c).start()

    def send_last(p):
        remote(st1.at[last, :, cut(1 - core, p), :], bufs[p].at[pl.ds(2 * me, 2)],
               one_sem.at[0, p], one_sem.at[1, p], other).start()

    def finish_two(t):
        finish(2 * t + 1)
        finish(2 * t)
        for u in (3, 2):
            @pl.when(2 * t + u < last)
            def _():
                for c in range(2):
                    send_one(2 * t + u, c, 0)

    def swap_back(q):
        part = pl.ds(q * CHUNK, CHUNK)
        return remote(gh.at[core, part], gh.at[core, part], swg_s.at[q], swg_r.at[q], other)

    def swapped(q):
        part = pl.ds(q * CHUNK, CHUNK)
        return remote(gh.at[1 - core, part], gh.at[1 - core, part], swg_s.at[q], swg_r.at[q], other)

    rounds = chips // CHUNK
    for q in range(rounds - 1, -2, -1):
        if q >= 0:
            each(q * CHUNK, min(q * CHUNK + CHUNK, last), arrived)
            swap_back(q).start()
        if q < rounds - 1:
            swapped(q + 1).wait_recv()
            each(0, CHUNK // 2, lambda t: finish_two((q + 2) * CHUNK // 2 - 1 - t))
    for p in range(PARTS):
        bufs[p][pl.ds(2 * me, 2)] = st1[last, :, cut(core, p), :]
    for q in range(4):
        for copy in swap(q):
            copy.wait_send()
    for q in range(rounds):
        swap_back(q).wait_send()
    for h in range(2):
        part = (pl.ds(0, last), quarter(h))
        remote(gs.at[part], gs.at[part], back_s.at[h], back_r.at[h, 0], other).wait_send()
    for j in (1, 0):
        for c in range(2):
            send_one(j, c, 0)
    send_last(0)
    for p in range(1, PARTS):
        def rest(i):
            for c in range(2):
                send_one(i, c, p)

        each(0, last, rest)
        send_last(p)
    remote(ordv.at[pl.ds(0, n - 1)], ordv.at[pl.ds(0, n - 1)], osem.at[0], osem.at[1], other).wait()
    to_scalars = pltpu.make_async_copy(ordv, ordsm, gsem.at[11])
    to_scalars.start()
    to_scalars.wait()

    def send_two(i, p):
        remote(perms[p].at[i], out_ref.at[:, cut(core, p), lanes_of(chip)],
               two_sem.at[0, p], two_sem.at[1, p], device_at(i)).start()

    for p in range(PARTS):
        arrivals = remote(bufs[p].at[pl.ds(0, 2 * n - 2)], bufs[p].at[pl.ds(0, 2 * n - 2)],
                          one_sem.at[0, p], one_sem.at[1, p], other)
        arrivals.wait()

        def pick_and_send(i):
            to = device_at(i)
            for b in range(2):
                perms[p][i, b] = bufs[p][ordsm[to, 0, b]]

            @pl.when(i > 0)
            def _():
                send_two(i - 1, p)

        each(0, n - 1, pick_and_send)
        for b in range(2):
            out_ref[b, cut(core, p), lanes_of(chip)] = bufs[p][ordsm[me, 0, b]]
        send_two(n - 2, p)
    for p in range(PARTS):
        sent = perms[p].at[pl.ds(0, n - 1)]
        remote(sent, sent, two_sem.at[0, p], two_sem.at[1, p], other).wait()
        if p == 0:
            loads[10].wait()

            def norm_some(i):
                rows = pl.ds(pl.multiple_of(i % 2 * 64, 64), SPLIT[0])
                out_ref[i // 2, rows, :] = normed(out_ref[i // 2, rows, :], gain_ref[...])

            each(0, 4, norm_some)


def normed(v, gain):
    v = v.astype(F32)
    mean = jnp.mean(v * v, axis=-1, keepdims=True)
    return (v * lax.rsqrt(mean + 1e-05) * gain).astype(BF16)


def norm_kernel(v_ref, w_ref, o_hbm, o_v, sem):
    def done(i):
        rows = pl.ds(pl.multiple_of(i % 2 * 64, 64), SPLIT[0])
        return pltpu.make_async_copy(v_ref.at[i // 2, rows], o_hbm.at[i // 2, rows], sem.at[i])

    def late(i):
        return pl.ds(pl.multiple_of(i % 2 * 64 + SPLIT[0], 16), SPLIT[1])

    def store(i):
        return pltpu.make_async_copy(o_v.at[i], o_hbm.at[i // 2, late(i)], sem.at[i + 4])

    each(0, 4, lambda i: done(i).start())

    def body(i):
        o_v[i] = normed(v_ref[i // 2, late(i), :], w_ref[...])
        store(i).start()

    each(0, 4, body)
    each(0, 4, lambda i: done(i).wait())
    each(0, 4, lambda i: store(i).wait())


def local(head_input, gate_input, write_vector, read_vector, increment_preactivation, step_bias,
          decay_log, skip_gain, norm_weight, doc_starts, block_order):
    n = lax.axis_size("ctx")
    chips = n // 2
    tokens, width = head_input.shape
    vmem = pl.BlockSpec(memory_space=pltpu.VMEM)
    hbm = pl.BlockSpec(memory_space=pltpu.HBM)
    dma = pltpu.SemaphoreType.DMA
    routed = pl.pallas_call(
        functools.partial(mega_kernel, n),
        out_shape=jax.ShapeDtypeStruct((2, GROUP, width), BF16),
        in_specs=[hbm] * 11,
        out_specs=vmem,
        scratch_shapes=[
            pltpu.SMEM((2,), jnp.int32),
            pltpu.SMEM((2,), jnp.int32),
            pltpu.VMEM((tokens, STATE), BF16),
            pltpu.VMEM((tokens, STATE), BF16),
            pltpu.VMEM((HEAD_DIM, tokens), BF16),
            pltpu.VMEM((1, HEAD_DIM), F32),
            pltpu.VMEM((1, HEAD_DIM), F32),
            pltpu.VMEM((1, HEAD_DIM), F32),
            pltpu.VMEM((1, width), F32),
            pltpu.VMEM((tokens, HEAD_DIM), F32),
            pltpu.VMEM((tokens, HEAD_DIM), F32),
            pltpu.VMEM((tokens, width), BF16),
            pltpu.VMEM((tokens, width), BF16),
            pltpu.VMEM((chips, tokens, LANES), F32),
            pltpu.VMEM((chips, STATE, LANES), F32),
            pltpu.VMEM((chips, STATE, LANES), BF16),
            pltpu.VMEM((chips, STATE, LANES), BF16),
            pltpu.VMEM((chips, 1, LANES), F32),
            pltpu.VMEM((chips, 1, LANES), F32),
            pltpu.VMEM((chips, 64, LANES), BF16),
            pltpu.VMEM((chips, 1, LANES), F32),
            pltpu.VMEM((chips, 64, LANES), BF16),
            pltpu.VMEM((chips, 1, LANES), F32),
            pltpu.VMEM((chips, 64, LANES), BF16),
            pltpu.VMEM((2, chips, 64, LANES), BF16),
            pltpu.VMEM((chips, 2, GROUP, LANES), BF16),
            pltpu.VMEM((2 * n, SPLIT[0], LANES), BF16),
            pltpu.VMEM((2 * n, SPLIT[1], LANES), BF16),
            pltpu.VMEM((n, 2, SPLIT[0], LANES), BF16),
            pltpu.VMEM((n, 2, SPLIT[1], LANES), BF16),
            pltpu.VMEM((1, LANES), jnp.int32),
            pltpu.VMEM((n, 1, LANES), jnp.int32),
            pltpu.SMEM((n, 1, LANES), jnp.int32),
            pltpu.VMEM((2 * GROUP, 192), BF16),
            pltpu.VMEM((272, 2 * HEAD_DIM), BF16),
            pltpu.VMEM((2 * HEAD_DIM, GROUP), F32),
            pltpu.VMEM((2 * HEAD_DIM, GROUP), F32),
            pltpu.VMEM((2 * STATE, GROUP), F32),
            pltpu.VMEM((2 * GROUP, GROUP), F32),
            dma((12,)), dma((2,)), dma((4,)), dma((4,)), dma((4,)), dma((4,)), dma((2, 3)),
            dma((2,)), dma((2, chips)), dma((chips // CHUNK,)), dma((chips // CHUNK,)), dma((2, PARTS)), dma((2, PARTS)),
        ],
        compiler_params=pltpu.CompilerParams(
            collective_id=1, has_side_effects=True, vmem_limit_bytes=40 * 1024 * 1024),
        name="layer",
    )(*[pltpu.with_memory_space_constraint(v, pltpu.HBM) for v in (
        doc_starts, block_order, head_input, gate_input, write_vector, read_vector, increment_preactivation.T,
        step_bias[None], decay_log[None], skip_gain[None], norm_weight[None])])
    out = pl.pallas_call(
        norm_kernel,
        out_shape=jax.ShapeDtypeStruct((2, GROUP, width), BF16),
        in_specs=[vmem, vmem],
        out_specs=pl.BlockSpec(memory_space=pl.ANY),
        scratch_shapes=[pltpu.VMEM((4, SPLIT[1], width), BF16), dma((8,))],
        compiler_params=pltpu.CompilerParams(vmem_limit_bytes=8 * 1024 * 1024),
        name="gated_norm",
    )(routed, norm_weight[None])
    return out.reshape(tokens, width)


def solution(mesh):
    return jax.shard_map(
        local,
        mesh=mesh,
        in_specs=(
            P(("dp", "ctx"), None),
            P(("dp", "ctx"), None),
            P(("dp", "ctx"), None),
            P(("dp", "ctx"), None),
            P(("dp", "ctx"), None),
            P(),
            P(),
            P(),
            P(),
            P(("dp", "ctx")),
            P(("dp", "ctx")),
        ),
        out_specs=P(("dp", "ctx"), None),
        check_vma=False,
    )
```

```python
import functools

import jax
import jax.numpy as jnp
from jax import lax
from jax.experimental import pallas as pl
from jax.experimental.pallas import tpu as pltpu
from jax.sharding import PartitionSpec as P

GROUP = 128
HEAD_DIM = 64
STATE = 128
LANES = 128
LOG2E = 1.4426950408889634
F32 = jnp.float32
BF16 = jnp.bfloat16
MESH = pl.DeviceIdType.MESH


def high(v):
    return v.astype(BF16).astype(F32)


def split2(v):
    hi = high(v)
    return hi.astype(BF16), (v - hi).astype(BF16)


def split3(v):
    hi = high(v)
    mid = high(v - hi)
    return hi.astype(BF16), mid.astype(BF16), (v - hi - mid).astype(BF16)


def dot(a, b):
    return jnp.dot(a, b, preferred_element_type=F32)


def iota(shape, dim):
    return lax.broadcasted_iota(jnp.int32, shape, dim)


def picks_two(k):
    shape = (2 * HEAD_DIM, LANES)
    return ((iota(shape, 0) & 63) == 2 * k + (iota(shape, 1) >> 6)).astype(BF16)


def picks_three(k):
    shape = (192, 2 * LANES)
    return ((iota(shape, 0) & 63) == 2 * k + (iota(shape, 1) >> 7)).astype(BF16)


def remote(src, dst, send, recv, device):
    return pltpu.make_async_remote_copy(
        src_ref=src, dst_ref=dst, send_sem=send, recv_sem=recv,
        device_id={"ctx": device}, device_id_type=MESH)


def around(i, n):
    return jnp.where(i == n - 1, 0, jnp.where((i & 1) == 0, i // 2 + 1, n - (i + 1) // 2))


def each(lo, hi, act, step=1):
    def body(i, carry):
        for u in range(step):
            act(lo + i * step + u)
        return carry

    lax.fori_loop(0, (hi - lo) // step, body, 0)


WIDE = 4
SPLIT = (32, 32)
PARTS = len(SPLIT)
W0, W1 = 12, 22
CHUNK = 2


def mega_kernel(n, starts_hbm, mine_hbm, x_hbm, gate_hbm, b_hbm, c_hbm, inc_hbm, bias_hbm, decay_hbm, skip_hbm, gain_hbm, out_ref,
                starts_ref, mine_ref, b_ref, c_ref, inc_ref, bias_ref, decay_ref, skip_ref, gain_ref, cum_s, step_s, x_ref, gate_v, m_s, s0_s, f_s, pf, d_s, pd, fc, dc, rf, rd, gs, gh, st1, buf0, buf1, perm0, perm1,
                ordrow, ordv, ordsm, col_s, exp_s, row_s, tail_s, bt_s, sc_s,
                gsem, osem, swf_s, swf_r, swd_s, swd_r, out_sem, back_s, back_r, swg_s, swg_r, one_sem, two_sem):
    me = lax.axis_index("ctx")
    chip, core = me // 2, me % 2
    chips = n // 2
    last = chips - 1
    other = chip * 2 + (1 - core)
    first = core == 0

    def shifted(j, sign):
        return lax.rem(chip + sign * around(j, chips) + chips, chips)

    def pair_at(j):
        return shifted(j, -1)

    def device_at(i):
        return lax.rem(me + around(i, n), n)

    def lanes_of(k):
        return pl.ds(pl.multiple_of(k * LANES, LANES), LANES)

    def half_of(c):
        return pl.ds(pl.multiple_of(c * 64, 64), 64)

    loads = [pltpu.make_async_copy(src, dst, gsem.at[i]) for i, (src, dst) in enumerate((
        (inc_hbm, inc_ref), (bias_hbm, bias_ref), (decay_hbm, decay_ref), (b_hbm, b_ref), (starts_hbm, starts_ref),
        (skip_hbm, skip_ref), (x_hbm, x_ref), (mine_hbm, mine_ref), (c_hbm, c_ref), (gate_hbm, gate_v), (gain_hbm, gain_ref)))]
    for copy in loads[:3]:
        copy.start()
    barrier = pltpu.get_barrier_semaphore()
    depth = chips // WIDE
    x_at, z_at = chip // depth, chip % depth

    def hops(at):
        return min(at[0], WIDE - at[0]) + min(at[1], depth - at[1])

    def signal(device):
        pl.semaphore_signal(barrier, inc=1, device_id={"ctx": device}, device_id_type=MESH)

    for dx, dz in sorted(((dx, dz) for dx in range(WIDE) for dz in range(depth)), key=hops, reverse=True)[:last]:
        peer = 2 * (lax.rem(x_at + dx, WIDE) * depth + lax.rem(z_at + dz, depth))
        signal(peer)
        signal(peer + 1)
    signal(other)
    for copy in loads[3:]:
        copy.start()

    tri = (iota((GROUP, GROUP), 0) >= iota((GROUP, GROUP), 1))
    ones = tri.astype(F32)
    for copy in loads[:3]:
        copy.wait()
    v = inc_ref[...].astype(F32).T + bias_ref[...]
    step = jnp.maximum(v, 0.0) + jnp.log(1.0 + jnp.exp(-jnp.abs(v)))
    step_s[...] = step
    fall = -step * jnp.exp(decay_ref[...])
    ends, tails = [], []
    for b in range(2):
        rows = slice(b * GROUP, (b + 1) * GROUP)
        cum = jnp.dot(ones, fall[rows, :], preferred_element_type=F32, precision=lax.Precision.HIGHEST)
        cum_s[rows, :] = cum
        ends.append(cum[GROUP - 1:GROUP, :])
        tails.append(jnp.exp(ends[b] - cum) * step[rows, :])
    tail_s[...] = jnp.concatenate(tails, axis=1).T
    for copy in loads[3:6]:
        copy.wait()
    keep0 = 1.0 - starts_ref[0].astype(F32)
    keep1 = 1.0 - starts_ref[1].astype(F32)
    for b in range(2):
        rows = slice(b * GROUP, (b + 1) * GROUP)
        bt_s[rows, :] = b_ref[rows, :].astype(F32).T
    r16 = iota((16, HEAD_DIM), 0)
    small = jnp.where(r16 == 0, keep0 * jnp.exp(ends[0]), jnp.where(
        r16 == 1, keep1 * jnp.exp(ends[1]), jnp.where(r16 == 2, skip_ref[...], 0.0)))
    exp_s[pl.ds(256, 16), :] = jnp.concatenate(split2(small), axis=1)
    loads[7].wait()
    lane = iota((1, LANES), 1)
    ordrow[...] = jnp.where(lane == 0, mine_ref[0], mine_ref[1])
    ordv[me] = jnp.where(lane == 0, mine_ref[0], mine_ref[1])

    left = iota((GROUP, LANES), 1) < HEAD_DIM
    loads[6].wait()

    def states_of(j):
        k = pair_at(j)
        lanes = lanes_of(k)
        pick = picks_two(k)
        ends = dot(exp_s[pl.ds(256, 16), :], pick)
        a0, a1 = ends[0:1, :], ends[1:2, :]
        states = []
        for b in range(2):
            rows = slice(b * GROUP, (b + 1) * GROUP)
            both = jnp.concatenate(
                [bt_s[rows, :] * tail_s[pl.ds(b * HEAD_DIM + 2 * k + e, 1), :] for e in range(2)], axis=0)
            out = dot(both.astype(BF16), x_ref[rows, lanes])
            states.append(jnp.where(left, out[:STATE], out[STATE:]))
        s0_s[j] = states[0]
        f_s[j] = (a1 * states[0] + states[1]).astype(BF16)
        d_s[j] = a0 * a1

    def swap(q):
        part = pl.ds(q * 8, 8)
        return (remote(f_s.at[part], pf.at[part], swf_s.at[q], swf_r.at[q], other),
                remote(d_s.at[part], pd.at[part], swd_s.at[q], swd_r.at[q], other))

    def begin(q):
        for copy in swap(q):
            copy.start()

    half = half_of(core)

    def join(j):
        mine, theirs = f_s[j, half, :].astype(F32), pf[j, half, :].astype(F32)
        dm, dt = d_s[j], pd[j]
        f0, f1 = jnp.where(first, mine, theirs), jnp.where(first, theirs, mine)
        fc[j] = (jnp.where(first, dt, dm) * f0 + f1).astype(BF16)
        dc[j] = dm * dt

    def quarter(h):
        return pl.ds(h * 32, 32)

    def send_state(j, h):
        to = 2 * pair_at(j) + core
        remote(fc.at[j, quarter(h)], rf.at[chip, quarter(h)], out_sem.at[0, h], out_sem.at[1, h], to).start()
        if h == 0:
            remote(dc.at[j], rd.at[chip], out_sem.at[0, 2], out_sem.at[1, 2], to).start()

    def join_chunk(q):
        for copy in swap(q):
            copy.wait_recv()
        each(q * 8, q * 8 + 8, join, 2)
        each(q * 8, min(q * 8 + 8, last), lambda j: send_state(j, 0))

    for q in range(4):
        each(q * 8, q * 8 + 8, states_of, 2)
        if q == 1:
            pl.semaphore_wait(barrier, n - 1)
            begin(0)
            begin(1)
            each(1, n, lambda t: remote(
                ordrow, ordv.at[me], osem.at[0], osem.at[1], lax.rem(me + t, n)).start())
        elif q > 1:
            join_chunk(q - 2)
            begin(q)
    join_chunk(2)
    loads[8].wait()
    logs = []
    for b in range(2):
        rows = slice(b * GROUP, (b + 1) * GROUP)
        cum = cum_s[rows, :]
        exp_s[rows, :] = jnp.concatenate(split2(jnp.exp(cum)), axis=1)
        col_s[rows, :] = jnp.concatenate(split3(cum * LOG2E), axis=1)
        logs.append((jnp.log(step_s[rows, :]) - cum) * LOG2E)
        sc_s[rows, :] = lax.dot_general(
            c_ref[rows, :], b_ref[rows, :], (((1,), (1,)), ((), ())), preferred_element_type=F32)
    row_s[...] = jnp.concatenate(logs, axis=1).T
    join_chunk(3)
    each(0, last, lambda j: send_state(j, 1))
    rf[chip] = fc[last]
    rd[chip] = dc[last]

    def local_of(j):
        k = pair_at(j)
        lanes = lanes_of(k)
        col = dot(col_s[...], picks_three(k))
        gain = dot(exp_s[pl.ds(256, 16), :], picks_two(k))[2:3, :]
        for b in range(2):
            rows = slice(b * GROUP, (b + 1) * GROUP)
            xb = x_ref[rows, lanes]
            outs = []
            for e in range(2):
                gap = col[rows, e * LANES:(e + 1) * LANES] + row_s[pl.ds(b * HEAD_DIM + 2 * k + e, 1), :]
                w = jnp.exp2(jnp.where(tri, gap, -1e30)) * sc_s[rows, :]
                outs.append(dot(w.astype(BF16), xb))
            m_s[j, rows, :] = jnp.where(left, outs[0], outs[1]) + gain * xb.astype(F32)

    def received(h):
        part = (pl.ds(0, last), quarter(h))
        remote(fc.at[part], rf.at[part], out_sem.at[0, h], out_sem.at[1, h], other).wait()

    def walk(h):
        def one(s, g):
            gs[s, quarter(h), :] = g.astype(BF16)
            return rd[s] * g + rf[s, quarter(h), :].astype(F32)

        lax.fori_loop(0, chips, one, jnp.zeros((32, LANES), F32))
        gh[core, last, quarter(h), :] = gs[chip, quarter(h), :]

    def send_back(i, h):
        s = shifted(i, 1)
        remote(gs.at[s, quarter(h)], gh.at[core, i, quarter(h)], back_s.at[h], back_r.at[h, i], 2 * s + core).start()

    each(0, W0, local_of, 2)
    remote(dc.at[pl.ds(0, last)], rd.at[pl.ds(0, last)], out_sem.at[0, 2], out_sem.at[1, 2], other).wait()
    received(0)
    walk(0)
    each(0, last, lambda t: send_back(last - 1 - t, 0))
    each(W0, W1, local_of, 2)
    received(1)
    walk(1)
    each(0, last, lambda t: send_back(last - 1 - t, 1))
    each(W1, chips, local_of, 2)
    loads[9].wait()

    def arrived(i):
        for h in range(2):
            remote(gs.at[0, quarter(h)], gh.at[core, i, quarter(h)], back_s.at[h], back_r.at[h, i], other).wait_recv()

    def finish(i):
        k = pair_at(i)
        lanes = lanes_of(k)
        pick = picks_two(k)
        ex = dot(exp_s[...], pick)
        a0 = ex[256:257, :]
        g = jnp.concatenate([gh[0, i], gh[1, i]], axis=0).astype(F32)
        g = jnp.where(first, g, pd[i] * g + pf[i].astype(F32))
        after = a0 * g + s0_s[i]
        entering = ((keep0 * g).astype(BF16), (keep1 * after).astype(BF16))
        for b in range(2):
            rows = slice(b * GROUP, (b + 1) * GROUP)
            mixed = m_s[i, rows, :] + ex[rows, :] * dot(c_ref[rows, :], entering[b])
            z = gate_v[rows, lanes].astype(F32)
            st1[i, b] = (mixed * (z / (1.0 + jnp.exp(-z)))).astype(BF16)

    bufs, perms = (buf0, buf1), (perm0, perm1)

    def cut(c, p):
        return pl.ds(pl.multiple_of(c * 64 + sum(SPLIT[:p]), 16), SPLIT[p])

    def send_one(i, c, p):
        remote(st1.at[i, :, cut(c, p), :], bufs[p].at[pl.ds(2 * me, 2)],
               one_sem.at[0, p], one_sem.at[1, p], 2 * pair_at(i) + c).start()

    def send_last(p):
        remote(st1.at[last, :, cut(1 - core, p), :], bufs[p].at[pl.ds(2 * me, 2)],
               one_sem.at[0, p], one_sem.at[1, p], other).start()

    def finish_two(t):
        finish(2 * t + 1)
        finish(2 * t)
        for u in (3, 2):
            @pl.when(2 * t + u < last)
            def _():
                for c in range(2):
                    send_one(2 * t + u, c, 0)

    def swap_back(q):
        part = pl.ds(q * CHUNK, CHUNK)
        return remote(gh.at[core, part], gh.at[core, part], swg_s.at[q], swg_r.at[q], other)

    def swapped(q):
        part = pl.ds(q * CHUNK, CHUNK)
        return remote(gh.at[1 - core, part], gh.at[1 - core, part], swg_s.at[q], swg_r.at[q], other)

    rounds = chips // CHUNK
    for q in range(rounds - 1, -2, -1):
        if q >= 0:
            each(q * CHUNK, min(q * CHUNK + CHUNK, last), arrived)
            swap_back(q).start()
        if q < rounds - 1:
            swapped(q + 1).wait_recv()
            each(0, CHUNK // 2, lambda t: finish_two((q + 2) * CHUNK // 2 - 1 - t))
    for p in range(PARTS):
        bufs[p][pl.ds(2 * me, 2)] = st1[last, :, cut(core, p), :]
    for q in range(4):
        for copy in swap(q):
            copy.wait_send()
    for q in range(rounds):
        swap_back(q).wait_send()
    for h in range(2):
        part = (pl.ds(0, last), quarter(h))
        remote(gs.at[part], gs.at[part], back_s.at[h], back_r.at[h, 0], other).wait_send()
    for j in (1, 0):
        for c in range(2):
            send_one(j, c, 0)
    send_last(0)
    for p in range(1, PARTS):
        def rest(i):
            for c in range(2):
                send_one(i, c, p)

        each(0, last, rest)
        send_last(p)
    remote(ordv.at[pl.ds(0, n - 1)], ordv.at[pl.ds(0, n - 1)], osem.at[0], osem.at[1], other).wait()
    to_scalars = pltpu.make_async_copy(ordv, ordsm, gsem.at[11])
    to_scalars.start()
    to_scalars.wait()

    def send_two(i, p):
        remote(perms[p].at[i], out_ref.at[:, cut(core, p), lanes_of(chip)],
               two_sem.at[0, p], two_sem.at[1, p], device_at(i)).start()

    for p in range(PARTS):
        arrivals = remote(bufs[p].at[pl.ds(0, 2 * n - 2)], bufs[p].at[pl.ds(0, 2 * n - 2)],
                          one_sem.at[0, p], one_sem.at[1, p], other)
        arrivals.wait()

        def pick_and_send(i):
            to = device_at(i)
            for b in range(2):
                perms[p][i, b] = bufs[p][ordsm[to, 0, b]]

            @pl.when(i > 0)
            def _():
                send_two(i - 1, p)

        each(0, n - 1, pick_and_send)
        for b in range(2):
            out_ref[b, cut(core, p), lanes_of(chip)] = bufs[p][ordsm[me, 0, b]]
        send_two(n - 2, p)
    for p in range(PARTS):
        sent = perms[p].at[pl.ds(0, n - 1)]
        remote(sent, sent, two_sem.at[0, p], two_sem.at[1, p], other).wait()
        if p == 0:
            loads[10].wait()

            def norm_some(i):
                rows = pl.ds(pl.multiple_of(i % 2 * 64, 64), SPLIT[0])
                out_ref[i // 2, rows, :] = normed(out_ref[i // 2, rows, :], gain_ref[...])

            each(0, 4, norm_some)


def normed(v, gain):
    v = v.astype(F32)
    mean = jnp.mean(v * v, axis=-1, keepdims=True)
    return (v * lax.rsqrt(mean + 1e-05) * gain).astype(BF16)


def norm_kernel(v_ref, w_ref, o_hbm, o_v, sem):
    def done(i):
        rows = pl.ds(pl.multiple_of(i % 2 * 64, 64), SPLIT[0])
        return pltpu.make_async_copy(v_ref.at[i // 2, rows], o_hbm.at[i // 2, rows], sem.at[i])

    def late(i):
        return pl.ds(pl.multiple_of(i % 2 * 64 + SPLIT[0], 16), SPLIT[1])

    def store(i):
        return pltpu.make_async_copy(o_v.at[i], o_hbm.at[i // 2, late(i)], sem.at[i + 4])

    each(0, 4, lambda i: done(i).start())

    def body(i):
        o_v[i] = normed(v_ref[i // 2, late(i), :], w_ref[...])
        store(i).start()

    each(0, 4, body)
    each(0, 4, lambda i: done(i).wait())
    each(0, 4, lambda i: store(i).wait())


def local(head_input, gate_input, write_vector, read_vector, increment_preactivation, step_bias,
          decay_log, skip_gain, norm_weight, doc_starts, block_order):
    n = lax.axis_size("ctx")
    chips = n // 2
    tokens, width = head_input.shape
    vmem = pl.BlockSpec(memory_space=pltpu.VMEM)
    hbm = pl.BlockSpec(memory_space=pltpu.HBM)
    dma = pltpu.SemaphoreType.DMA
    routed = pl.pallas_call(
        functools.partial(mega_kernel, n),
        out_shape=jax.ShapeDtypeStruct((2, GROUP, width), BF16),
        in_specs=[hbm] * 11,
        out_specs=vmem,
        scratch_shapes=[
            pltpu.SMEM((2,), jnp.int32),
            pltpu.SMEM((2,), jnp.int32),
            pltpu.VMEM((tokens, STATE), BF16),
            pltpu.VMEM((tokens, STATE), BF16),
            pltpu.VMEM((HEAD_DIM, tokens), BF16),
            pltpu.VMEM((1, HEAD_DIM), F32),
            pltpu.VMEM((1, HEAD_DIM), F32),
            pltpu.VMEM((1, HEAD_DIM), F32),
            pltpu.VMEM((1, width), F32),
            pltpu.VMEM((tokens, HEAD_DIM), F32),
            pltpu.VMEM((tokens, HEAD_DIM), F32),
            pltpu.VMEM((tokens, width), BF16),
            pltpu.VMEM((tokens, width), BF16),
            pltpu.VMEM((chips, tokens, LANES), F32),
            pltpu.VMEM((chips, STATE, LANES), F32),
            pltpu.VMEM((chips, STATE, LANES), BF16),
            pltpu.VMEM((chips, STATE, LANES), BF16),
            pltpu.VMEM((chips, 1, LANES), F32),
            pltpu.VMEM((chips, 1, LANES), F32),
            pltpu.VMEM((chips, 64, LANES), BF16),
            pltpu.VMEM((chips, 1, LANES), F32),
            pltpu.VMEM((chips, 64, LANES), BF16),
            pltpu.VMEM((chips, 1, LANES), F32),
            pltpu.VMEM((chips, 64, LANES), BF16),
            pltpu.VMEM((2, chips, 64, LANES), BF16),
            pltpu.VMEM((chips, 2, GROUP, LANES), BF16),
            pltpu.VMEM((2 * n, SPLIT[0], LANES), BF16),
            pltpu.VMEM((2 * n, SPLIT[1], LANES), BF16),
            pltpu.VMEM((n, 2, SPLIT[0], LANES), BF16),
            pltpu.VMEM((n, 2, SPLIT[1], LANES), BF16),
            pltpu.VMEM((1, LANES), jnp.int32),
            pltpu.VMEM((n, 1, LANES), jnp.int32),
            pltpu.SMEM((n, 1, LANES), jnp.int32),
            pltpu.VMEM((2 * GROUP, 192), BF16),
            pltpu.VMEM((272, 2 * HEAD_DIM), BF16),
            pltpu.VMEM((2 * HEAD_DIM, GROUP), F32),
            pltpu.VMEM((2 * HEAD_DIM, GROUP), F32),
            pltpu.VMEM((2 * STATE, GROUP), F32),
            pltpu.VMEM((2 * GROUP, GROUP), F32),
            dma((12,)), dma((2,)), dma((4,)), dma((4,)), dma((4,)), dma((4,)), dma((2, 3)),
            dma((2,)), dma((2, chips)), dma((chips // CHUNK,)), dma((chips // CHUNK,)), dma((2, PARTS)), dma((2, PARTS)),
        ],
        compiler_params=pltpu.CompilerParams(
            collective_id=1, has_side_effects=True, vmem_limit_bytes=40 * 1024 * 1024),
        name="layer",
    )(*[pltpu.with_memory_space_constraint(v, pltpu.HBM) for v in (
        doc_starts, block_order, head_input, gate_input, write_vector, read_vector, increment_preactivation.T,
        step_bias[None], decay_log[None], skip_gain[None], norm_weight[None])])
    out = pl.pallas_call(
        norm_kernel,
        out_shape=jax.ShapeDtypeStruct((2, GROUP, width), BF16),
        in_specs=[vmem, vmem],
        out_specs=pl.BlockSpec(memory_space=pl.ANY),
        scratch_shapes=[pltpu.VMEM((4, SPLIT[1], width), BF16), dma((8,))],
        compiler_params=pltpu.CompilerParams(vmem_limit_bytes=8 * 1024 * 1024),
        name="gated_norm",
    )(routed, norm_weight[None])
    return out.reshape(tokens, width)


def solution(mesh):
    return jax.shard_map(
        local,
        mesh=mesh,
        in_specs=(
            P(("dp", "ctx"), None),
            P(("dp", "ctx"), None),
            P(("dp", "ctx"), None),
            P(("dp", "ctx"), None),
            P(("dp", "ctx"), None),
            P(),
            P(),
            P(),
            P(),
            P(("dp", "ctx")),
            P(("dp", "ctx")),
        ),
        out_specs=P(("dp", "ctx"), None),
        check_vma=False,
    )
```
